32 devices in a mesh: chan: 4 (over y, x), rows: 8 (over z, core).
Axes of the slice: x: 2, y: 2, z: 4, core: 2. Of those that a mesh axis runs over, the one named last changes fastest.
Arguments:
- residual: float32 [4, 256, 16384], P('chan', 'rows'), may hold values from -6 to 6
- psf: float32 [4, 2048, 2048], P('chan', 'rows'), may hold values from -2 to 2
- positions: int32 [32, 2], replicated, may hold values from 0 to 15360, as said below
Outputs:
- residual_out: float32 [4, 256, 16384], P('chan', 'rows')
- normalized: float32 [256, 16384], P('rows', 'chan')
The draws below stay inside these ranges and needn't reach their ends.
Inputs may be any that keep to these rules, and one draw needn't show every extreme that they name: positions[k, 0] is a row of the image, 0 to 255; positions[k, 1] is a column from 1024 to 15360.
All inputs are finite; a program needn't handle non-finite values.
Results may differ from the reference program's by a relative error of at most 0.0001.
Values sent between devices are 32-bit elements; how exact they have to be, the bound alone decides.
A program may use at most 128 MiB of HBM per device.

```python
import jax
import jax.numpy as jnp
from jax import lax

CHANNELS = 4
NCOL = 16384
PATCH = 2048
STEPS = 32
NX = 256


def draw_positions(key, part):
    half = PATCH // 2
    row_key = jax.random.fold_in(key, 11)
    col_key = jax.random.fold_in(key, 12)
    pick_key = jax.random.fold_in(key, 13)
    rows = jax.random.randint(row_key, (STEPS,), 0, NX)
    cols = jax.random.randint(col_key, (STEPS,), half, NCOL - half + 1)
    picks = jax.random.randint(pick_key, (2,), 0, STEPS)
    low_step = picks[0]
    high_step = (low_step + 1) % STEPS
    rows = rows.at[low_step].set(0)
    rows = rows.at[high_step].set(NX - 1)
    cols = cols.at[picks[1]].set(NCOL - half)
    return jnp.stack([rows, cols], axis=1).astype(jnp.int32)


def block_scale(key, shape, shards, least, largest):
    factor_of, own = 1.0, jax.random.fold_in(key, 6)
    for axis_at, parts in shards:
        draws = jnp.exp(jax.random.uniform(jax.random.fold_in(own, axis_at), (parts,), jnp.float32, least / len(shards), largest / len(shards)))
        factor_of = factor_of * jnp.repeat(draws, shape[axis_at] // parts).reshape([-1 if axis == axis_at else 1 for axis in range(len(shape))])
    return factor_of


def normal_values(key, extent, deviation, reach, pieces=(), dtype=jnp.bfloat16):
    array = deviation * jax.random.normal(key, extent, jnp.float32)
    if pieces:
        array = array * block_scale(key, extent, pieces, -0.22, 0.18)
    return jnp.clip(array, -reach, reach).astype(dtype)


def setup_inputs(seed: int = 0) -> dict:
    key_list = jax.random.split(jax.random.key(seed), 4)
    residual = normal_values(key_list[0], (CHANNELS, NX, NCOL), 1.0, 6.0, ((0, 4), (1, 8)), jnp.float32)
    psf = normal_values(key_list[1], (CHANNELS, PATCH, PATCH), 0.3, 2.0, ((0, 4), (1, 8)), jnp.float32)
    positions = draw_positions(jax.random.fold_in(key_list[3], 71), 0)
    return {"residual": residual, "psf": psf, "positions": positions}


def reference(residual, psf, positions):
    half = PATCH // 2
    padded = jnp.pad(residual, ((0, 0), (half, half), (0, 0)))
    zero = jnp.int32(0)

    def step(k, image):
        row = positions[k, 0].astype(jnp.int32)
        col = positions[k, 1].astype(jnp.int32)
        value = lax.dynamic_slice(image, (zero, row + half, col), (CHANNELS, 1, 1)).reshape(CHANNELS)
        total = jnp.sum(value)
        amp = 0.25 * (value + total / CHANNELS)
        window = lax.dynamic_slice(image, (zero, row, col - half), (CHANNELS, PATCH, PATCH))
        window = window - amp[:, None, None] * psf
        return lax.dynamic_update_slice(image, window, (zero, row, col - half))
    padded = lax.fori_loop(0, STEPS, step, padded)
    image = padded[:, half:half + NX, :]
    summed = lax.optimization_barrier(jnp.sum(image, axis=0))
    mean_square = jnp.mean(summed * summed)
    return (image, summed * lax.rsqrt(mean_square + 1e-06))
```

```python
import functools

import jax
import jax.numpy as jnp
from jax import lax
from jax.experimental import pallas as pl
from jax.experimental.pallas import tpu as pltpu
from jax.sharding import PartitionSpec as P

STEPS = 32
LANES = 128
PIECES = 4
MESH = pl.DeviceIdType.MESH


def at(start, size):
    return pl.ds(pl.multiple_of(start, 8), size)


def pick(ref, row, col, wanted, lane_to, acc):
    place = (pl.ds(pl.multiple_of((row >> 3) << 3, 8), 8), pl.ds(pl.multiple_of((col >> 7) << 7, LANES), LANES))
    tile = pltpu.roll(ref[place], (lane_to - col) & (LANES - 1), 1)
    number = lax.broadcasted_iota(jnp.int32, (8, LANES), 0) * LANES + lax.broadcasted_iota(jnp.int32, (8, LANES), 1)
    return jnp.where(number == jnp.where(wanted, (row & 7) * LANES + lane_to, -1), tile, acc)


def table_kernel(pos, res, psf, start, couple, res_v, psf_v, sems):
    row, nrows = lax.axis_index("rows"), lax.axis_size("rows")
    slab, steps = res.shape[1], pos.shape[0]
    shard, patch = psf.shape[1:]
    half = patch // 2
    first = row * slab
    is_root = jnp.logical_or(row == nrows // 2 - 1, row == nrows // 2)
    loads = [pltpu.make_async_copy(res.at[0], res_v, sems.at[0]), pltpu.make_async_copy(psf.at[0], psf_v, sems.at[1])]
    loads[0].start()

    @pl.when(is_root)
    def _():
        loads[1].start()

    loads[0].wait()
    acc = jnp.zeros((8, LANES), jnp.float32)
    for k in range(steps):
        r = pos[k, 0] - first
        inside = jnp.logical_and(r >= 0, r < slab)
        acc = pick(res_v, jnp.clip(r, 0, slab - 1), pos[k, 1], inside, k, acc)
    start[...] = acc

    @pl.when(is_root)
    def _():
        loads[1].wait()

        def fill(k, carry):
            line = jnp.zeros((8, LANES), jnp.float32)
            rk = pos[k, 0] + half - row * shard
            qk = pos[k, 1] + half
            for j in range(steps):
                r = rk - pos[j, 0]
                c = qk - pos[j, 1]
                owned = (r >= 0) & (r < shard) & (c >= 0) & (c < patch)
                line = pick(psf_v, jnp.clip(r, 0, shard - 1), jnp.clip(c, 0, patch - 1), owned, j, line)
            couple[pl.ds(k, 1), :] = jnp.sum(line, axis=0, keepdims=True)
            return carry

        lax.fori_loop(0, steps, fill, 0)

    @pl.when(jnp.logical_not(is_root))
    def _():
        couple[...] = jnp.zeros_like(couple)


def make_tables(positions, residual, psf):
    f32 = jnp.float32
    anywhere, vmem = pl.BlockSpec(memory_space=pl.ANY), pl.BlockSpec(memory_space=pltpu.VMEM)
    return pl.pallas_call(
        table_kernel,
        out_shape=(jax.ShapeDtypeStruct((8, LANES), f32), jax.ShapeDtypeStruct((positions.shape[0], LANES), f32)),
        in_specs=[pl.BlockSpec(memory_space=pltpu.SMEM), anywhere, anywhere],
        out_specs=(vmem, vmem),
        scratch_shapes=[pltpu.VMEM(residual.shape[1:], f32), pltpu.VMEM(psf.shape[1:], f32), pltpu.SemaphoreType.DMA((2,))],
        name="make_tables",
    )(positions, residual, psf)


def gather_kernel(nchan, nrows, psf, start_own, couple_own, win, amps_out, psf_v, couple_in, start_in, tables, amps_v,
                  load_sem, keep_sem, send_sem, recv_sem, pass_sem, start_send, start_recv, couple_sem, table_send, table_recv, amp_send, amp_recv):
    chan, row = lax.axis_index("chan"), lax.axis_index("rows")
    chip, core = row // 2, row % 2
    partner = row + 1 - 2 * core
    nchips = nrows // 2
    slab = psf.shape[1] // nrows
    unit = 2 * slab
    low, high = nchips - 1, nchips
    steps = couple_own.shape[0]
    lane = lax.broadcasted_iota(jnp.int32, (1, LANES), 1)

    load = pltpu.make_async_copy(psf.at[0], psf_v, load_sem)
    is_low, is_high = row == low, row == high
    is_root = jnp.logical_or(is_low, is_high)

    @pl.when(is_root)
    def _():
        load.start()

    barrier = pltpu.get_barrier_semaphore()
    for step in range(1, nrows):
        pl.semaphore_signal(barrier, inc=1, device_id=(chan, (row + step) % nrows), device_id_type=MESH)
    for step in range(1, nchan):
        pl.semaphore_signal(barrier, inc=1, device_id=((chan + step) % nchan, row), device_id_type=MESH)
    pl.semaphore_wait(barrier, nrows + nchan - 2)

    def piece(to_row, z, m, h, index):
        return pltpu.make_async_remote_copy(
            src_ref=psf.at[0, pl.ds(index, slab)], dst_ref=win.at[pl.ds(m * unit + h * slab, slab)],
            send_sem=send_sem.at[z, m, h], recv_sem=recv_sem.at[m, h], device_id=(chan, to_row), device_id_type=MESH)

    def pieces(root, zs):
        out = []
        for m in range(nchips + 1):
            for z in zs:
                if (z + m < nchips) != (root == low):
                    continue
                for h in range(2):
                    to_row = root ^ 1 if z == root // 2 else 2 * z + h
                    out.append(piece(to_row, z, m, h, ((z + m) % nchips) * unit + h * slab))
        return out

    away = {low: [z for z in range(nchips) if z < low // 2], high: [z for z in range(nchips) if z > high // 2]}
    back = {low: [z for z in range(nchips) if z >= low // 2], high: [z for z in range(nchips) if z <= high // 2]}

    def kept(root):
        z = root // 2
        out = []
        for m in range(nchips + 1):
            if (z + m < nchips) == (root == low):
                out.append(pltpu.make_async_copy(psf_v.at[pl.ds(((z + m) % nchips) * unit, unit)], win.at[pl.ds(m * unit, unit)], keep_sem.at[m]))
        return out

    for root in (low, high):
        @pl.when(row == root)
        def _(root=root):
            for copy in pieces(root, away[root]):
                copy.start()

    def start_copy(source):
        return pltpu.make_async_remote_copy(
            src_ref=start_own, dst_ref=start_in.at[source], send_sem=start_send, recv_sem=start_recv.at[source],
            device_id=(chan, low), device_id_type=MESH)

    @pl.when(jnp.logical_not(is_low))
    def _():
        start_copy(row).start()

    couple_copy = pltpu.make_async_remote_copy(
        src_ref=couple_own, dst_ref=couple_in, send_sem=couple_sem.at[0], recv_sem=couple_sem.at[1],
        device_id=(chan, low), device_id_type=MESH)

    @pl.when(is_high)
    def _():
        couple_copy.start()

    for root in (low, high):
        @pl.when(row == root)
        def _(root=root):
            for copy in pieces(root, back[root]):
                copy.start()
            load.wait()
            for copy in kept(root):
                copy.start()

    def amp_copy(step):
        return pltpu.make_async_remote_copy(
            src_ref=amps_v, dst_ref=amps_v, send_sem=amp_send.at[step], recv_sem=amp_recv,
            device_id=(chan, (low + step) % nrows), device_id_type=MESH)

    def table_copy(peer, owner):
        return pltpu.make_async_remote_copy(
            src_ref=tables.at[owner], dst_ref=tables.at[owner], send_sem=table_send.at[peer], recv_sem=table_recv.at[owner],
            device_id=(peer, low), device_id_type=MESH)

    def relay(m):
        block = at(m * unit + core * slab, slab)
        return pltpu.make_async_remote_copy(
            src_ref=win.at[block], dst_ref=win.at[block], send_sem=pass_sem.at[m], recv_sem=recv_sem.at[m, core],
            device_id=(chan, partner), device_id_type=MESH)

    def arrival(m, h):
        return pltpu.make_async_remote_copy(
            src_ref=win.at[at(m * unit + h * slab, slab)], dst_ref=win.at[at(m * unit + h * slab, slab)],
            send_sem=pass_sem.at[m], recv_sem=recv_sem.at[m, h], device_id=(chan, partner), device_id_type=MESH)

    @pl.when(is_low)
    def _():
        total = start_own[...]
        for step in range(1, nrows):
            source = (low + step) % nrows
            start_copy(source).wait_recv()
            total = total + start_in[source]
        couple_copy.wait_recv()
        tables[chan, pl.ds(0, steps), :] = couple_own[...] + couple_in[...]
        tables[chan, pl.ds(steps, 8), :] = jnp.broadcast_to(jnp.sum(total, axis=0, keepdims=True), total.shape)
        for step in range(1, nchan):
            table_copy((chan + step) % nchan, chan).start()
        for step in range(1, nchan):
            table_copy((chan + step) % nchan, (chan + step) % nchan).wait_recv()
        start = jnp.concatenate([tables[c, pl.ds(steps, 1), :] for c in range(nchan)], axis=0)

        def solve(k, amps):
            couple = jnp.concatenate([tables[c, pl.ds(k, 1), :] for c in range(nchan)], axis=0)
            value = jnp.sum(jnp.where(lane == k, start, 0.0) - amps * couple, axis=1, keepdims=True)
            amp = 0.25 * (value + jnp.sum(value, axis=0, keepdims=True) / nchan)
            return jnp.where(lane == k, amp, amps)

        amps = lax.fori_loop(0, steps, solve, jnp.zeros((nchan, LANES), jnp.float32))
        amps_v[pl.ds(0, nchan), :] = amps
        amps_v[pl.ds(nchan, 8 - nchan), :] = jnp.zeros((8 - nchan, LANES), jnp.float32)
        for step in range(1, nrows):
            amp_copy(step).start()

    for m in range(nchips + 1):
        root = jnp.where(chip + m < nchips, low, high)
        relays = jnp.logical_and(row != root, partner != root)

        @pl.when(relays)
        def _(m=m):
            arrival(m, core).wait_recv()
            relay(m).start()

    for m in range(nchips + 1):
        root = jnp.where(chip + m < nchips, low, high)

        @pl.when(jnp.logical_and(row != root, partner != root))
        def _(m=m):
            arrival(m, 1 - core).wait_recv()
            relay(m).wait_send()

        @pl.when(partner == root)
        def _(m=m):
            arrival(m, 0).wait_recv()
            arrival(m, 1).wait_recv()

    for root in (low, high):
        @pl.when(row == root)
        def _(root=root):
            for copy in kept(root):
                copy.wait()
            for copy in pieces(root, away[root]) + pieces(root, back[root]):
                copy.wait_send()

    @pl.when(is_high)
    def _():
        couple_copy.wait_send()

    @pl.when(is_low)
    def _():
        for step in range(1, nchan):
            table_copy((chan + step) % nchan, chan).wait_send()
        for step in range(1, nrows):
            amp_copy(step).wait_send()

    @pl.when(jnp.logical_not(is_low))
    def _():
        start_copy(row).wait_send()
        amp_copy(1).wait_recv()

    amps_out[...] = amps_v[...]


def gather_patch(nchan, nrows, psf, start, couple):
    shard, patch = psf.shape[1:]
    steps, slab = couple.shape[0], shard // nrows
    nchips = nrows // 2
    rows = slab * (nrows + 2)
    dma, f32 = pltpu.SemaphoreType.DMA, jnp.float32
    anywhere = pl.BlockSpec(memory_space=pl.ANY)
    return pl.pallas_call(
        functools.partial(gather_kernel, nchan, nrows),
        out_shape=(jax.ShapeDtypeStruct((rows, patch), f32), jax.ShapeDtypeStruct((8, LANES), f32)),
        in_specs=[anywhere, pl.BlockSpec(memory_space=pltpu.VMEM), pl.BlockSpec(memory_space=pltpu.VMEM)],
        out_specs=(anywhere, pl.BlockSpec(memory_space=pltpu.VMEM)),
        scratch_shapes=[
            pltpu.VMEM((shard, patch), f32), pltpu.VMEM((steps, LANES), f32), pltpu.VMEM((nrows, 8, LANES), f32),
            pltpu.VMEM((nchan, steps + 8, LANES), f32), pltpu.VMEM((8, LANES), f32),
            dma, dma((nchips + 1,)), dma((nchips, nchips + 1, 2)), dma((nchips + 1, 2)), dma((nchips + 1,)),
            dma, dma((nrows,)), dma((2,)), dma((nchan,)), dma((nchan,)), dma((nrows,)), dma,
        ],
        compiler_params=pltpu.CompilerParams(collective_id=0, has_side_effects=True),
        name="gather_patch",
    )(psf, start, couple)


def apply_kernel(pos, amps, res, win, out, image, patch_v, sems):
    chan, row = lax.axis_index("chan"), lax.axis_index("rows")
    nrows = lax.axis_size("rows")
    slab, ncols = res.shape[1], res.shape[2]
    rows, patch = win.shape
    chunks = patch // LANES
    loads = [pltpu.make_async_copy(win.at[:, pl.ds(c * LANES, LANES)], patch_v.at[c], sems.at[c]) for c in range(chunks)]
    loads.append(pltpu.make_async_copy(res.at[0], image.at[:, pl.ds(0, ncols)], sems.at[chunks]))
    for copy in loads:
        copy.start()
    for copy in loads:
        copy.wait()
    lane = lax.broadcasted_iota(jnp.int32, (8, LANES), 1)
    top = (row % 2) * slab + slab * nrows

    def step(k, carry):
        amp = amps[chan, k]
        begin = top - pos[k, 0]
        left = pos[k, 1] - patch // 2
        shift = left & (LANES - 1)
        base = left - shift
        keep = lane < shift
        for t in range(slab // 8):
            before = jnp.zeros((8, LANES), jnp.float32)
            for c in range(chunks + 1):
                now = jnp.zeros((8, LANES), jnp.float32)
                if c < chunks:
                    now = pltpu.roll(patch_v[c, pl.ds(begin + 8 * t, 8), :] * amp, shift, 1)
                place = (pl.ds(8 * t, 8), pl.ds(pl.multiple_of(base + c * LANES, LANES), LANES))
                image[place] = image[place] - jnp.where(keep, before, now)
                before = now
        return carry

    lax.fori_loop(0, pos.shape[0], step, 0)
    store = pltpu.make_async_copy(image.at[:, pl.ds(0, ncols)], out.at[0], sems.at[0])
    store.start()
    store.wait()


def apply_peaks(positions, amps, residual, win):
    slab, ncols = residual.shape[1:]
    rows, patch = win.shape
    chunks = patch // LANES
    anywhere, scalars = pl.BlockSpec(memory_space=pl.ANY), pl.BlockSpec(memory_space=pltpu.SMEM)
    return pl.pallas_call(
        apply_kernel,
        out_shape=jax.ShapeDtypeStruct(residual.shape, jnp.float32),
        in_specs=[scalars, scalars, anywhere, anywhere],
        out_specs=anywhere,
        scratch_shapes=[
            pltpu.VMEM((slab, ncols + LANES), jnp.float32), pltpu.VMEM((chunks, rows, LANES), jnp.float32),
            pltpu.SemaphoreType.DMA((chunks + 1,)),
        ],
        name="apply_peaks",
    )(positions, amps, residual, win)


def sum_kernel(nchan, nrows, count, image, out, own, near, first_far, first_own, passed, second, squares,
               load_sem, far_send, far_recv, own_send, own_recv, pass_send, pass_recv, square_send, square_recv):
    chan, row = lax.axis_index("chan"), lax.axis_index("rows")
    me = row * nchan + chan
    slab, ncols = image.shape[1], image.shape[2]
    cols = ncols // nchan
    part = slab // 2
    width = cols // PIECES
    bits = ((1, 2), (2, 1))

    def block(c):
        return pl.ds(pl.multiple_of(c * cols, LANES), cols)

    def flip(bit):
        if bit == 1:
            return chan + 1 - 2 * (chan % 2)
        return (chan + 2) % 4

    diagonal = 3 - chan
    loads = [pltpu.make_async_copy(image.at[0, :, block(chan)], own, load_sem.at[0])]
    for p in range(2):
        loads.append(pltpu.make_async_copy(image.at[0, pl.ds(p * part, part), block(flip(bits[p][1]))], near.at[p], load_sem.at[1 + p]))
    for copy in loads:
        copy.start()

    barrier = pltpu.get_barrier_semaphore()
    for step in range(1, nrows * nchan):
        other = (me + step) % (nrows * nchan)
        pl.semaphore_signal(barrier, inc=1, device_id=(other % nchan, other // nchan), device_id_type=MESH)
    pl.semaphore_wait(barrier, nrows * nchan - 1)

    def send(p, g, source, dest, send_sem, recv_sem, to):
        return pltpu.make_async_remote_copy(
            src_ref=source, dst_ref=dest.at[p, :, pl.ds(g * width, width)], send_sem=send_sem.at[p, g], recv_sem=recv_sem.at[p, g],
            device_id=(to, row), device_id_type=MESH)

    def tile(p, g, c):
        return image.at[0, pl.ds(p * part, part), pl.ds(pl.multiple_of(c * cols + g * width, LANES), width)]

    def far(p, g):
        return send(p, g, tile(p, g, diagonal), first_far, far_send, far_recv, flip(bits[p][0]))

    def mine(p, g):
        return send(p, g, tile(p, g, flip(bits[p][0])), first_own, own_send, own_recv, flip(bits[p][0]))

    def onward(p, g):
        return send(p, g, passed.at[p, :, pl.ds(g * width, width)], second, pass_send, pass_recv, flip(bits[p][1]))

    for g in range(PIECES):
        for p in range(2):
            far(p, g).start()
    for g in range(PIECES):
        for p in range(2):
            mine(p, g).start()
    for copy in loads:
        copy.wait()
    for g in range(PIECES):
        for p in range(2):
            span = pl.ds(g * width, width)
            far(p, g).wait_recv()
            passed[p, :, span] = near[p, :, span] + first_far[p, :, span]
            onward(p, g).start()
    for g in range(PIECES):
        for p in range(2):
            span = pl.ds(g * width, width)
            mine(p, g).wait_recv()
            rows = pl.ds(p * part, part)
            own[rows, span] = own[rows, span] + first_own[p, :, span]
    total = jnp.zeros((8, LANES), jnp.float32)
    for g in range(PIECES):
        for p in range(2):
            span = pl.ds(g * width, width)
            onward(p, g).wait_recv()
            rows = pl.ds(p * part, part)
            value = own[rows, span] + second[p, :, span]
            own[rows, span] = value
            square = value * value
            for t in range(part // 8):
                for c in range(width // LANES):
                    total = total + square[8 * t:8 * t + 8, c * LANES:(c + 1) * LANES]
    squares[pl.ds(me, 1), :] = jnp.sum(total, axis=0, keepdims=True)

    def spread(step):
        other = (me + step) % (nrows * nchan)
        return pltpu.make_async_remote_copy(
            src_ref=squares.at[pl.ds(me, 1)], dst_ref=squares.at[pl.ds(me, 1)], send_sem=square_send.at[step], recv_sem=square_recv.at[step],
            device_id=(other % nchan, other // nchan), device_id_type=MESH)

    def arrived(step):
        other = (me + nrows * nchan - step) % (nrows * nchan)
        return pltpu.make_async_remote_copy(
            src_ref=squares.at[pl.ds(other, 1)], dst_ref=squares.at[pl.ds(other, 1)], send_sem=square_send.at[step], recv_sem=square_recv.at[step],
            device_id=(other % nchan, other // nchan), device_id_type=MESH)

    for step in range(1, nrows * nchan):
        spread(step).start()
    for step in range(1, nrows * nchan):
        arrived(step).wait_recv()
    everything = jnp.sum(jnp.sum(squares[...], axis=0, keepdims=True), axis=1, keepdims=True)
    scale = lax.rsqrt(everything / count + 1e-06)
    out[...] = own[...] * scale
    for step in range(1, nrows * nchan):
        spread(step).wait_send()
    for g in range(PIECES):
        for p in range(2):
            far(p, g).wait_send()
            mine(p, g).wait_send()
            onward(p, g).wait_send()


def sum_channels(nchan, nrows, image):
    slab, ncols = image.shape[1:]
    cols, part = ncols // nchan, slab // 2
    dma, f32 = pltpu.SemaphoreType.DMA, jnp.float32
    halves = pltpu.VMEM((2, part, cols), f32)
    return pl.pallas_call(
        functools.partial(sum_kernel, nchan, nrows, slab * nrows * ncols),
        out_shape=jax.ShapeDtypeStruct((slab, cols), f32),
        in_specs=[pl.BlockSpec(memory_space=pl.ANY)],
        out_specs=pl.BlockSpec(memory_space=pltpu.VMEM),
        scratch_shapes=[pltpu.VMEM((slab, cols), f32)] + [halves] * 5 + [pltpu.VMEM((nrows * nchan, LANES), f32), dma((3,))]
        + [dma((2, PIECES))] * 6 + [dma((nrows * nchan,))] * 2,
        compiler_params=pltpu.CompilerParams(collective_id=1, has_side_effects=True),
        name="sum_channels",
    )(image)


def on_device(residual, psf, positions):
    nchan, nrows = lax.axis_size("chan"), lax.axis_size("rows")
    slab, ncols = residual.shape[1:]
    shard, patch = psf.shape[1:]
    central = nrows % 2 == 0 and slab * nrows == shard and 2 * shard * (nrows // 2) == patch
    if not (central and nchan == 4 and slab % 16 == 0 and positions.shape[0] % 8 == 0 and positions.shape[0] <= LANES):
        return on_any_device(residual, psf, positions)
    start, couple = make_tables(positions, residual, psf)
    win, amps = gather_patch(nchan, nrows, psf, start, couple)
    image = apply_peaks(positions, amps, residual, win)
    return (image, sum_channels(nchan, nrows, image))


def on_any_device(residual, psf, positions):
    chan_id = lax.axis_index("chan")
    nchan = lax.axis_size("chan")
    row_id = lax.axis_index("rows")
    nrows = lax.axis_size("rows")
    slab = residual.shape[1]
    ncols = residual.shape[2]
    own_psf = psf[0]
    shard_rows = own_psf.shape[0]
    patch = own_psf.shape[1]
    half = patch // 2
    first = row_id * slab
    chan_hot = (jnp.arange(nchan) == chan_id).astype(jnp.float32)
    full_psf = lax.all_gather(own_psf, "rows", axis=0, tiled=True)
    padded_psf = jnp.pad(full_psf, ((slab, slab), (0, 0)))
    zero = jnp.int32(0)

    def subtract(image, row, col, amount):
        offset = first - row + half
        touches = jnp.logical_and(offset > -slab, offset < patch)
        start = jnp.clip(offset + slab, 0, patch + slab)
        psf_rows = lax.dynamic_slice(padded_psf, (start, zero), (slab, patch))
        window = lax.dynamic_slice(image, (zero, col - half), (slab, patch))
        scale = jnp.where(touches, amount, 0.0)
        return lax.dynamic_update_slice(image, window - scale * psf_rows, (zero, col - half))

    image = residual[0]
    peak_rows = positions[:, 0]
    peak_cols = positions[:, 1]
    inside = jnp.logical_and(peak_rows >= first, peak_rows < first + slab)
    local_rows = jnp.clip(peak_rows - first, 0, slab - 1)
    start_values = jnp.where(inside, image[local_rows, peak_cols], 0.0)
    row_offset = peak_rows[:, None] - peak_rows[None, :] + half - row_id * shard_rows
    col_offset = peak_cols[:, None] - peak_cols[None, :] + half
    owned = (row_offset >= 0) & (row_offset < shard_rows) & (col_offset >= 0) & (col_offset < patch)
    couple = own_psf[jnp.clip(row_offset, 0, shard_rows - 1), jnp.clip(col_offset, 0, patch - 1)]
    couple = jnp.where(owned, couple, 0.0)
    start_table, couple_table = lax.psum(
        (chan_hot[:, None] * start_values[None, :], chan_hot[:, None, None] * couple[None, :, :]),
        ("chan", "rows"),
    )

    def solve(k, amps):
        taken = jnp.sum(amps * lax.dynamic_index_in_dim(couple_table, k, 1, False), axis=1)
        value = lax.dynamic_index_in_dim(start_table, k, 1, False) - taken
        amp = 0.25 * (value + jnp.sum(value) / nchan)
        return lax.dynamic_update_index_in_dim(amps, amp, k, 1)

    amps = lax.fori_loop(0, STEPS, solve, jnp.zeros((nchan, STEPS), jnp.float32))
    own_amps = jnp.sum(chan_hot[:, None] * amps, axis=0)

    def apply(k, image):
        return subtract(image, positions[k, 0], positions[k, 1], own_amps[k])

    image = lax.fori_loop(0, STEPS, apply, image)
    count = slab * nrows * ncols
    parts = lax.psum_scatter(image, "chan", scatter_dimension=1, tiled=True)
    total = lax.psum(jnp.sum(parts * parts), ("chan", "rows"))
    normalized = parts * lax.rsqrt(total / count + 1e-06)
    return (image[None], normalized)


def solution(mesh):
    return jax.shard_map(
        on_device,
        mesh=mesh,
        in_specs=(P("chan", "rows", None), P("chan", "rows", None), P()),
        out_specs=(P("chan", "rows", None), P("rows", "chan")),
        check_vma=False,
    )
```

```python
import functools

import jax
import jax.numpy as jnp
from jax import lax
from jax.experimental import pallas as pl
from jax.experimental.pallas import tpu as pltpu
from jax.sharding import PartitionSpec as P

STEPS = 32
LANES = 128
PIECES = 4
MESH = pl.DeviceIdType.MESH


def at(start, size):
    return pl.ds(pl.multiple_of(start, 8), size)


def aligned(row, col):
    return (pl.ds(pl.multiple_of((row >> 3) << 3, 8), 8), pl.ds(pl.multiple_of((col >> 7) << 7, LANES), LANES))


def pick(tile, row, col, lane_to, number, acc):
    moved = pltpu.roll(tile, (lane_to - col) & (LANES - 1), 1)
    return jnp.where(number == (row & 7) * LANES + lane_to, moved, acc)


def table_kernel(pos, res, psf, start, couple, tiles, psf_v, load_sem, sems):
    row, nrows = lax.axis_index("rows"), lax.axis_size("rows")
    slab, steps = res.shape[1], pos.shape[1]
    shard, patch = psf.shape[1:]
    half = patch // 2
    first = row * slab
    is_root = jnp.logical_or(row == nrows // 2 - 1, row == nrows // 2)
    load = pltpu.make_async_copy(psf.at[0], psf_v, load_sem)

    @pl.when(is_root)
    def _():
        load.start()

    loads = []
    for k in range(steps):
        rows, cols = aligned(jnp.clip(pos[0, k] - first, 0, slab - 1), pos[1, k])
        loads.append(pltpu.make_async_copy(res.at[0, rows, cols], tiles.at[k], sems.at[k]))
    for copy in loads:
        copy.start()
    lane = lax.broadcasted_iota(jnp.int32, (1, LANES), 1)
    number = lax.broadcasted_iota(jnp.int32, (8, LANES), 0) * LANES + lax.broadcasted_iota(jnp.int32, (8, LANES), 1)
    peak_rows, peak_cols = jnp.zeros((1, LANES), jnp.int32), jnp.zeros((1, LANES), jnp.int32)
    for k in range(steps):
        peak_rows = jnp.where(lane == k, pos[0, k], peak_rows)
        peak_cols = jnp.where(lane == k, pos[1, k], peak_cols)
    for copy in loads:
        copy.wait()
    acc = jnp.zeros((8, LANES), jnp.float32)
    for k in range(steps):
        acc = pick(tiles[k], pos[0, k] - first, pos[1, k], k, number, acc)
    inside = (peak_rows >= first) & (peak_rows < first + slab) & (lane < steps)
    start[...] = jnp.where(inside, acc, 0.0)

    @pl.when(is_root)
    def _():
        load.wait()

        def fill(k, carry):
            rk = pos[0, k] + half - row * shard
            qk = pos[1, k] + half

            def group(g, line):
                for i in range(8):
                    j = g * 8 + i
                    r = (rk - pos[0, j]) & (shard - 1)
                    c = (qk - pos[1, j]) & (patch - 1)
                    line = pick(psf_v[aligned(r, c)], r, c, j, number, line)
                return line

            line = lax.fori_loop(0, (k + 7) >> 3, group, jnp.zeros((8, LANES), jnp.float32))
            r, c = rk - peak_rows, qk - peak_cols
            owned = (r >= 0) & (r < shard) & (c >= 0) & (c < patch) & (lane < k)
            couple[pl.ds(k, 1), :] = jnp.where(owned, jnp.sum(line, axis=0, keepdims=True), 0.0)
            return carry

        lax.fori_loop(0, steps, fill, 0)

    @pl.when(jnp.logical_not(is_root))
    def _():
        couple[...] = jnp.zeros_like(couple)


def make_tables(positions, residual, psf):
    f32 = jnp.float32
    anywhere, vmem = pl.BlockSpec(memory_space=pl.ANY), pl.BlockSpec(memory_space=pltpu.VMEM)
    return pl.pallas_call(
        table_kernel,
        out_shape=(jax.ShapeDtypeStruct((8, LANES), f32), jax.ShapeDtypeStruct((positions.shape[1], LANES), f32)),
        in_specs=[pl.BlockSpec(memory_space=pltpu.SMEM), anywhere, anywhere],
        out_specs=(vmem, vmem),
        scratch_shapes=[
            pltpu.VMEM((positions.shape[1], 8, LANES), f32), pltpu.VMEM(psf.shape[1:], f32),
            pltpu.SemaphoreType.DMA, pltpu.SemaphoreType.DMA((positions.shape[1],)),
        ],
        name="make_tables",
    )(positions, residual, psf)


def gather_kernel(nchan, nrows, psf, start_own, couple_own, win, amps_out, psf_v, couple_in, start_in, tables, amps_v,
                  load_sem, keep_sem, send_sem, recv_sem, pass_sem, start_send, start_recv, couple_sem, table_send, table_recv, amp_send, amp_recv):
    chan, row = lax.axis_index("chan"), lax.axis_index("rows")
    chip, core = row // 2, row % 2
    partner = row + 1 - 2 * core
    nchips = nrows // 2
    slab = psf.shape[1] // nrows
    unit = 2 * slab
    low, high = nchips - 1, nchips
    steps = couple_own.shape[0]
    lane = lax.broadcasted_iota(jnp.int32, (1, LANES), 1)

    load = pltpu.make_async_copy(psf.at[0], psf_v, load_sem)
    is_low, is_high = row == low, row == high
    is_root = jnp.logical_or(is_low, is_high)

    @pl.when(is_root)
    def _():
        load.start()

    barrier = pltpu.get_barrier_semaphore()
    for step in range(1, nrows):
        pl.semaphore_signal(barrier, inc=1, device_id=(chan, (row + step) % nrows), device_id_type=MESH)
    for step in range(1, nchan):
        pl.semaphore_signal(barrier, inc=1, device_id=((chan + step) % nchan, row), device_id_type=MESH)
    pl.semaphore_wait(barrier, nrows + nchan - 2)

    def piece(to_row, z, m, h, index):
        return pltpu.make_async_remote_copy(
            src_ref=psf.at[0, pl.ds(index, slab)], dst_ref=win.at[pl.ds(m * unit + h * slab, slab)],
            send_sem=send_sem.at[z, m, h], recv_sem=recv_sem.at[m, h], device_id=(chan, to_row), device_id_type=MESH)

    def pieces(root, zs):
        out = []
        for m in range(nchips + 1):
            for z in zs:
                if (z + m < nchips) != (root == low):
                    continue
                for h in range(2):
                    to_row = root ^ 1 if z == root // 2 else 2 * z + h
                    out.append(piece(to_row, z, m, h, ((z + m) % nchips) * unit + h * slab))
        return out

    away = {low: [z for z in range(nchips) if z < low // 2], high: [z for z in range(nchips) if z > high // 2]}
    back = {low: [z for z in range(nchips) if z >= low // 2], high: [z for z in range(nchips) if z <= high // 2]}

    def kept(root):
        z = root // 2
        out = []
        for m in range(nchips + 1):
            if (z + m < nchips) == (root == low):
                out.append(pltpu.make_async_copy(psf_v.at[pl.ds(((z + m) % nchips) * unit, unit)], win.at[pl.ds(m * unit, unit)], keep_sem.at[m]))
        return out

    for root in (low, high):
        @pl.when(row == root)
        def _(root=root):
            for copy in pieces(root, away[root]):
                copy.start()

    def start_copy(source):
        return pltpu.make_async_remote_copy(
            src_ref=start_own, dst_ref=start_in.at[source], send_sem=start_send, recv_sem=start_recv.at[source],
            device_id=(chan, low), device_id_type=MESH)

    @pl.when(jnp.logical_not(is_low))
    def _():
        start_copy(row).start()

    couple_copy = pltpu.make_async_remote_copy(
        src_ref=couple_own, dst_ref=couple_in, send_sem=couple_sem.at[0], recv_sem=couple_sem.at[1],
        device_id=(chan, low), device_id_type=MESH)

    @pl.when(is_high)
    def _():
        couple_copy.start()

    for root in (low, high):
        @pl.when(row == root)
        def _(root=root):
            for copy in pieces(root, back[root]):
                copy.start()
            load.wait()
            for copy in kept(root):
                copy.start()

    def amp_copy(step):
        return pltpu.make_async_remote_copy(
            src_ref=amps_v, dst_ref=amps_v, send_sem=amp_send.at[step], recv_sem=amp_recv,
            device_id=(chan, (low + step) % nrows), device_id_type=MESH)

    def table_copy(peer, owner):
        return pltpu.make_async_remote_copy(
            src_ref=tables.at[owner], dst_ref=tables.at[owner], send_sem=table_send.at[peer], recv_sem=table_recv.at[owner],
            device_id=(peer, low), device_id_type=MESH)

    def relay(m):
        block = at(m * unit + core * slab, slab)
        return pltpu.make_async_remote_copy(
            src_ref=win.at[block], dst_ref=win.at[block], send_sem=pass_sem.at[m], recv_sem=recv_sem.at[m, core],
            device_id=(chan, partner), device_id_type=MESH)

    def arrival(m, h):
        return pltpu.make_async_remote_copy(
            src_ref=win.at[at(m * unit + h * slab, slab)], dst_ref=win.at[at(m * unit + h * slab, slab)],
            send_sem=pass_sem.at[m], recv_sem=recv_sem.at[m, h], device_id=(chan, partner), device_id_type=MESH)

    @pl.when(is_low)
    def _():
        total = start_own[...]
        for step in range(1, nrows):
            source = (low + step) % nrows
            start_copy(source).wait_recv()
            total = total + start_in[source]
        couple_copy.wait_recv()
        tables[chan, pl.ds(0, steps), :] = couple_own[...] + couple_in[...]
        tables[chan, pl.ds(steps, 8), :] = jnp.broadcast_to(jnp.sum(total, axis=0, keepdims=True), total.shape)
        for step in range(1, nchan):
            table_copy((chan + step) % nchan, chan).start()
        for step in range(1, nchan):
            table_copy((chan + step) % nchan, (chan + step) % nchan).wait_recv()
        start = jnp.concatenate([tables[c, pl.ds(steps, 1), :] for c in range(nchan)], axis=0)

        def solve(k, amps):
            couple = jnp.concatenate([tables[c, pl.ds(k, 1), :] for c in range(nchan)], axis=0)
            value = jnp.sum(jnp.where(lane == k, start, 0.0) - amps * couple, axis=1, keepdims=True)
            amp = 0.25 * (value + jnp.sum(value, axis=0, keepdims=True) / nchan)
            return jnp.where(lane == k, amp, amps)

        amps = lax.fori_loop(0, steps, solve, jnp.zeros((nchan, LANES), jnp.float32))
        amps_v[pl.ds(0, nchan), :] = amps
        amps_v[pl.ds(nchan, 8 - nchan), :] = jnp.zeros((8 - nchan, LANES), jnp.float32)
        for step in range(1, nrows):
            amp_copy(step).start()

    for m in range(nchips + 1):
        root = jnp.where(chip + m < nchips, low, high)
        relays = jnp.logical_and(row != root, partner != root)

        @pl.when(relays)
        def _(m=m):
            arrival(m, core).wait_recv()
            relay(m).start()

    for m in range(nchips + 1):
        root = jnp.where(chip + m < nchips, low, high)

        @pl.when(jnp.logical_and(row != root, partner != root))
        def _(m=m):
            arrival(m, 1 - core).wait_recv()
            relay(m).wait_send()

        @pl.when(partner == root)
        def _(m=m):
            arrival(m, 0).wait_recv()
            arrival(m, 1).wait_recv()

    for root in (low, high):
        @pl.when(row == root)
        def _(root=root):
            for copy in kept(root):
                copy.wait()
            for copy in pieces(root, away[root]) + pieces(root, back[root]):
                copy.wait_send()

    @pl.when(is_high)
    def _():
        couple_copy.wait_send()

    @pl.when(is_low)
    def _():
        for step in range(1, nchan):
            table_copy((chan + step) % nchan, chan).wait_send()
        for step in range(1, nrows):
            amp_copy(step).wait_send()

    @pl.when(jnp.logical_not(is_low))
    def _():
        start_copy(row).wait_send()
        amp_copy(1).wait_recv()

    amps_out[...] = amps_v[...]


def gather_patch(nchan, nrows, psf, start, couple):
    shard, patch = psf.shape[1:]
    steps, slab = couple.shape[0], shard // nrows
    nchips = nrows // 2
    rows = slab * (nrows + 2)
    dma, f32 = pltpu.SemaphoreType.DMA, jnp.float32
    anywhere = pl.BlockSpec(memory_space=pl.ANY)
    return pl.pallas_call(
        functools.partial(gather_kernel, nchan, nrows),
        out_shape=(jax.ShapeDtypeStruct((rows, patch), f32), jax.ShapeDtypeStruct((8, LANES), f32)),
        in_specs=[anywhere, pl.BlockSpec(memory_space=pltpu.VMEM), pl.BlockSpec(memory_space=pltpu.VMEM)],
        out_specs=(anywhere, pl.BlockSpec(memory_space=pltpu.VMEM)),
        scratch_shapes=[
            pltpu.VMEM((shard, patch), f32), pltpu.VMEM((steps, LANES), f32), pltpu.VMEM((nrows, 8, LANES), f32),
            pltpu.VMEM((nchan, steps + 8, LANES), f32), pltpu.VMEM((8, LANES), f32),
            dma, dma((nchips + 1,)), dma((nchips, nchips + 1, 2)), dma((nchips + 1, 2)), dma((nchips + 1,)),
            dma, dma((nrows,)), dma((2,)), dma((nchan,)), dma((nchan,)), dma((nrows,)), dma,
        ],
        compiler_params=pltpu.CompilerParams(collective_id=0, has_side_effects=True),
        name="gather_patch",
    )(psf, start, couple)


def apply_kernel(pos, amps, res, win, out, image, patch_v, sems):
    chan, row = lax.axis_index("chan"), lax.axis_index("rows")
    nrows = lax.axis_size("rows")
    slab, ncols = res.shape[1], res.shape[2]
    rows, patch = win.shape
    chunks = patch // LANES
    tiles = slab // 8
    loads = [pltpu.make_async_copy(win.at[:, pl.ds(c * LANES, LANES)], patch_v.at[c], sems.at[c]) for c in range(chunks)]

    def band(t):
        return pltpu.make_async_copy(res.at[0, pl.ds(8 * t, 8)], image.at[pl.ds(8 * t, 8), pl.ds(0, ncols)], sems.at[chunks + t])

    def done(t):
        return pltpu.make_async_copy(image.at[pl.ds(8 * t, 8), pl.ds(0, ncols)], out.at[0, pl.ds(8 * t, 8)], sems.at[chunks + tiles + t])

    band(0).start()
    for copy in loads:
        copy.start()
    for t in range(1, tiles):
        band(t).start()
    for copy in loads:
        copy.wait()
    lane = lax.broadcasted_iota(jnp.int32, (8, LANES), 1)
    top = (row % 2) * slab + slab * nrows

    for t in range(tiles):
        band(t).wait()

        def step(k, carry, t=t):
            amp = amps[chan, k]
            begin = top - pos[0, k] + 8 * t
            left = pos[1, k] - patch // 2
            shift = left & (LANES - 1)
            base = left - shift
            keep = lane < shift
            moved = [pltpu.roll(patch_v[c, pl.ds(begin, 8), :] * amp, shift, 1) for c in range(chunks)]
            places = [(pl.ds(8 * t, 8), pl.ds(pl.multiple_of(base + c * LANES, LANES), LANES)) for c in range(chunks + 1)]
            values = [image[place] for place in places]
            zero = jnp.zeros((8, LANES), jnp.float32)
            for c, place in enumerate(places):
                before = moved[c - 1] if c else zero
                now = moved[c] if c < chunks else zero
                values[c] = values[c] - jnp.where(keep, before, now)
            for c, place in enumerate(places):
                image[place] = values[c]
            return carry

        lax.fori_loop(0, pos.shape[1], step, 0)
        done(t).start()
    for t in range(tiles):
        done(t).wait()


def apply_peaks(positions, amps, residual, win):
    slab, ncols = residual.shape[1:]
    rows, patch = win.shape
    chunks = patch // LANES
    anywhere, scalars = pl.BlockSpec(memory_space=pl.ANY), pl.BlockSpec(memory_space=pltpu.SMEM)
    return pl.pallas_call(
        apply_kernel,
        out_shape=jax.ShapeDtypeStruct(residual.shape, jnp.float32),
        in_specs=[scalars, scalars, anywhere, anywhere],
        out_specs=anywhere,
        scratch_shapes=[
            pltpu.VMEM((slab, ncols + LANES), jnp.float32), pltpu.VMEM((chunks, rows, LANES), jnp.float32),
            pltpu.SemaphoreType.DMA((chunks + slab // 4,)),
        ],
        name="apply_peaks",
    )(positions, amps, residual, win)


def sum_kernel(nchan, nrows, image, out, total_out, own, near, first_far, first_own, passed, second, squares,
               load_sem, far_send, far_recv, own_send, own_recv, pass_send, pass_recv, square_send, square_recv):
    chan, row = lax.axis_index("chan"), lax.axis_index("rows")
    me = row * nchan + chan
    slab, ncols = image.shape[1], image.shape[2]
    cols = ncols // nchan
    part = slab // 2
    width = cols // PIECES
    bits = ((1, 2), (2, 1))

    def block(c):
        return pl.ds(pl.multiple_of(c * cols, LANES), cols)

    def flip(bit):
        if bit == 1:
            return chan + 1 - 2 * (chan % 2)
        return (chan + 2) % 4

    diagonal = 3 - chan
    loads = [pltpu.make_async_copy(image.at[0, :, block(chan)], own, load_sem.at[0])]
    for p in range(2):
        loads.append(pltpu.make_async_copy(image.at[0, pl.ds(p * part, part), block(flip(bits[p][1]))], near.at[p], load_sem.at[1 + p]))
    for copy in loads:
        copy.start()

    barrier = pltpu.get_barrier_semaphore()
    for step in range(1, nrows * nchan):
        other = (me + step) % (nrows * nchan)
        pl.semaphore_signal(barrier, inc=1, device_id=(other % nchan, other // nchan), device_id_type=MESH)
    pl.semaphore_wait(barrier, nrows * nchan - 1)

    def send(p, g, source, dest, send_sem, recv_sem, to):
        return pltpu.make_async_remote_copy(
            src_ref=source, dst_ref=dest.at[p, :, pl.ds(g * width, width)], send_sem=send_sem.at[p, g], recv_sem=recv_sem.at[p, g],
            device_id=(to, row), device_id_type=MESH)

    def tile(p, g, c):
        return image.at[0, pl.ds(p * part, part), pl.ds(pl.multiple_of(c * cols + g * width, LANES), width)]

    def far(p, g):
        return send(p, g, tile(p, g, diagonal), first_far, far_send, far_recv, flip(bits[p][0]))

    def mine(p, g):
        return send(p, g, tile(p, g, flip(bits[p][0])), first_own, own_send, own_recv, flip(bits[p][0]))

    def onward(p, g):
        return send(p, g, passed.at[p, :, pl.ds(g * width, width)], second, pass_send, pass_recv, flip(bits[p][1]))

    for g in range(PIECES):
        for p in range(2):
            far(p, g).start()
    for g in range(PIECES):
        for p in range(2):
            mine(p, g).start()
    for copy in loads:
        copy.wait()
    for g in range(PIECES):
        for p in range(2):
            span = pl.ds(g * width, width)
            far(p, g).wait_recv()
            passed[p, :, span] = near[p, :, span] + first_far[p, :, span]
            onward(p, g).start()
    for g in range(PIECES):
        for p in range(2):
            span = pl.ds(g * width, width)
            mine(p, g).wait_recv()
            rows = pl.ds(p * part, part)
            own[rows, span] = own[rows, span] + first_own[p, :, span]
    total = jnp.zeros((8, LANES), jnp.float32)
    for g in range(PIECES):
        for p in range(2):
            span = pl.ds(g * width, width)
            onward(p, g).wait_recv()
            rows = pl.ds(p * part, part)
            value = own[rows, span] + second[p, :, span]
            own[rows, span] = value
            square = value * value
            for t in range(part // 8):
                for c in range(width // LANES):
                    total = total + square[8 * t:8 * t + 8, c * LANES:(c + 1) * LANES]
    squares[pl.ds(me, 1), :] = jnp.sum(total, axis=0, keepdims=True)

    def spread(step):
        other = (me + step) % (nrows * nchan)
        return pltpu.make_async_remote_copy(
            src_ref=squares.at[pl.ds(me, 1)], dst_ref=squares.at[pl.ds(me, 1)], send_sem=square_send.at[step], recv_sem=square_recv.at[step],
            device_id=(other % nchan, other // nchan), device_id_type=MESH)

    def arrived(step):
        other = (me + nrows * nchan - step) % (nrows * nchan)
        return pltpu.make_async_remote_copy(
            src_ref=squares.at[pl.ds(other, 1)], dst_ref=squares.at[pl.ds(other, 1)], send_sem=square_send.at[step], recv_sem=square_recv.at[step],
            device_id=(other % nchan, other // nchan), device_id_type=MESH)

    for step in range(1, nrows * nchan):
        spread(step).start()
    keep = pltpu.make_async_copy(own, out, load_sem.at[0])
    keep.start()
    for step in range(1, nrows * nchan):
        arrived(step).wait_recv()
    everything = jnp.sum(jnp.sum(squares[...], axis=0, keepdims=True), axis=1, keepdims=True)
    total_out[...] = jnp.broadcast_to(everything, total_out.shape)
    keep.wait()
    for step in range(1, nrows * nchan):
        spread(step).wait_send()
    for g in range(PIECES):
        for p in range(2):
            far(p, g).wait_send()
            mine(p, g).wait_send()
            onward(p, g).wait_send()


def sum_channels(nchan, nrows, image):
    slab, ncols = image.shape[1:]
    cols, part = ncols // nchan, slab // 2
    dma, f32 = pltpu.SemaphoreType.DMA, jnp.float32
    halves = pltpu.VMEM((2, part, cols), f32)
    parts, total = pl.pallas_call(
        functools.partial(sum_kernel, nchan, nrows),
        out_shape=(jax.ShapeDtypeStruct((slab, cols), f32), jax.ShapeDtypeStruct((8, LANES), f32)),
        in_specs=[pl.BlockSpec(memory_space=pl.ANY)],
        out_specs=(pl.BlockSpec(memory_space=pl.ANY), pl.BlockSpec(memory_space=pltpu.VMEM)),
        scratch_shapes=[pltpu.VMEM((slab, cols), f32)] + [halves] * 5 + [pltpu.VMEM((nrows * nchan, LANES), f32), dma((3,))]
        + [dma((2, PIECES))] * 6 + [dma((nrows * nchan,))] * 2,
        compiler_params=pltpu.CompilerParams(collective_id=1, has_side_effects=True),
        name="sum_channels",
    )(image)
    return parts * lax.rsqrt(total[0, 0] / (slab * nrows * ncols) + 1e-06)


def on_device(residual, psf, positions):
    nchan, nrows = lax.axis_size("chan"), lax.axis_size("rows")
    slab, ncols = residual.shape[1:]
    shard, patch = psf.shape[1:]
    central = nrows % 2 == 0 and slab * nrows == shard and 2 * shard * (nrows // 2) == patch
    powers = shard & (shard - 1) == 0 and patch & (patch - 1) == 0
    if not (central and powers and nchan == 4 and slab % 16 == 0 and positions.shape[0] % 8 == 0 and positions.shape[0] <= LANES):
        return on_any_device(residual, psf, positions)
    positions = positions.T
    start, couple = make_tables(positions, residual, psf)
    win, amps = gather_patch(nchan, nrows, psf, start, couple)
    image = apply_peaks(positions, amps, residual, win)
    return (image, sum_channels(nchan, nrows, image))


def on_any_device(residual, psf, positions):
    chan_id = lax.axis_index("chan")
    nchan = lax.axis_size("chan")
    row_id = lax.axis_index("rows")
    nrows = lax.axis_size("rows")
    slab = residual.shape[1]
    ncols = residual.shape[2]
    own_psf = psf[0]
    shard_rows = own_psf.shape[0]
    patch = own_psf.shape[1]
    half = patch // 2
    first = row_id * slab
    chan_hot = (jnp.arange(nchan) == chan_id).astype(jnp.float32)
    full_psf = lax.all_gather(own_psf, "rows", axis=0, tiled=True)
    padded_psf = jnp.pad(full_psf, ((slab, slab), (0, 0)))
    zero = jnp.int32(0)

    def subtract(image, row, col, amount):
        offset = first - row + half
        touches = jnp.logical_and(offset > -slab, offset < patch)
        start = jnp.clip(offset + slab, 0, patch + slab)
        psf_rows = lax.dynamic_slice(padded_psf, (start, zero), (slab, patch))
        window = lax.dynamic_slice(image, (zero, col - half), (slab, patch))
        scale = jnp.where(touches, amount, 0.0)
        return lax.dynamic_update_slice(image, window - scale * psf_rows, (zero, col - half))

    image = residual[0]
    peak_rows = positions[:, 0]
    peak_cols = positions[:, 1]
    inside = jnp.logical_and(peak_rows >= first, peak_rows < first + slab)
    local_rows = jnp.clip(peak_rows - first, 0, slab - 1)
    start_values = jnp.where(inside, image[local_rows, peak_cols], 0.0)
    row_offset = peak_rows[:, None] - peak_rows[None, :] + half - row_id * shard_rows
    col_offset = peak_cols[:, None] - peak_cols[None, :] + half
    owned = (row_offset >= 0) & (row_offset < shard_rows) & (col_offset >= 0) & (col_offset < patch)
    couple = own_psf[jnp.clip(row_offset, 0, shard_rows - 1), jnp.clip(col_offset, 0, patch - 1)]
    couple = jnp.where(owned, couple, 0.0)
    start_table, couple_table = lax.psum(
        (chan_hot[:, None] * start_values[None, :], chan_hot[:, None, None] * couple[None, :, :]),
        ("chan", "rows"),
    )

    def solve(k, amps):
        taken = jnp.sum(amps * lax.dynamic_index_in_dim(couple_table, k, 1, False), axis=1)
        value = lax.dynamic_index_in_dim(start_table, k, 1, False) - taken
        amp = 0.25 * (value + jnp.sum(value) / nchan)
        return lax.dynamic_update_index_in_dim(amps, amp, k, 1)

    amps = lax.fori_loop(0, STEPS, solve, jnp.zeros((nchan, STEPS), jnp.float32))
    own_amps = jnp.sum(chan_hot[:, None] * amps, axis=0)

    def apply(k, image):
        return subtract(image, positions[k, 0], positions[k, 1], own_amps[k])

    image = lax.fori_loop(0, STEPS, apply, image)
    count = slab * nrows * ncols
    parts = lax.psum_scatter(image, "chan", scatter_dimension=1, tiled=True)
    total = lax.psum(jnp.sum(parts * parts), ("chan", "rows"))
    normalized = parts * lax.rsqrt(total / count + 1e-06)
    return (image[None], normalized)


def solution(mesh):
    return jax.shard_map(
        on_device,
        mesh=mesh,
        in_specs=(P("chan", "rows", None), P("chan", "rows", None), P()),
        out_specs=(P("chan", "rows", None), P("rows", "chan")),
        check_vma=False,
    )
```

```python
import functools

import jax
import jax.numpy as jnp
from jax import lax
from jax.experimental import pallas as pl
from jax.experimental.pallas import tpu as pltpu
from jax.sharding import PartitionSpec as P

STEPS = 32
LANES = 128
PIECES = 4
MESH = pl.DeviceIdType.MESH


def at(start, size):
    return pl.ds(pl.multiple_of(start, 8), size)


def aligned(row, col):
    return (pl.ds(pl.multiple_of((row >> 3) << 3, 8), 8), pl.ds(pl.multiple_of((col >> 7) << 7, LANES), LANES))


def pick(tile, row, col, lane_to, number, acc):
    moved = pltpu.roll(tile, (lane_to - col) & (LANES - 1), 1)
    return jnp.where(number == (row & 7) * LANES + lane_to, moved, acc)


def table_kernel(pos, res, psf, start, couple, tiles, psf_v, grid, pairs, load_sem, sems):
    row, nrows = lax.axis_index("rows"), lax.axis_size("rows")
    slab, steps = res.shape[1], pos.shape[1]
    shard, patch = psf.shape[1:]
    half = patch // 2
    first = row * slab
    is_root = jnp.logical_or(row == nrows // 2 - 1, row == nrows // 2)
    load = pltpu.make_async_copy(psf.at[0], psf_v, load_sem)

    @pl.when(is_root)
    def _():
        load.start()

    loads = []
    for k in range(steps):
        rows, cols = aligned(jnp.clip(pos[0, k] - first, 0, slab - 1), pos[1, k])
        loads.append(pltpu.make_async_copy(res.at[0, rows, cols], tiles.at[k], sems.at[k]))
    for copy in loads:
        copy.start()
    lane = lax.broadcasted_iota(jnp.int32, (1, LANES), 1)
    number = lax.broadcasted_iota(jnp.int32, (8, LANES), 0) * LANES + lax.broadcasted_iota(jnp.int32, (8, LANES), 1)
    peak_rows, peak_cols = jnp.zeros((1, LANES), jnp.int32), jnp.zeros((1, LANES), jnp.int32)
    for k in range(steps):
        peak_rows = jnp.where(lane == k, pos[0, k], peak_rows)
        peak_cols = jnp.where(lane == k, pos[1, k], peak_cols)
    for copy in loads:
        copy.wait()
    acc = jnp.zeros((8, LANES), jnp.float32)
    for k in range(steps):
        acc = pick(tiles[k], pos[0, k] - first, pos[1, k], k, number, acc)
    inside = (peak_rows >= first) & (peak_rows < first + slab) & (lane < steps)
    start[...] = jnp.where(inside, acc, 0.0)

    @pl.when(is_root)
    def _():
        grid[...] = jnp.zeros_like(grid)
        low = row * shard - half

        def listed(k, found):
            rk, qk = pos[0, k] - low, pos[1, k] + half

            def test(j, found):
                r, c = rk - pos[0, j], qk - pos[1, j]
                owned = (r >= 0) & (r < shard) & (c >= 0) & (c < patch)
                pairs[found] = k * steps + j
                return found + owned.astype(jnp.int32)

            return lax.fori_loop(0, k, test, found)

        found = lax.fori_loop(0, steps, listed, jnp.int32(0))
        load.wait()

        def fill(n, carry):
            k, j = pairs[n] // steps, pairs[n] % steps
            r, c = pos[0, k] - low - pos[0, j], pos[1, k] + half - pos[1, j]
            grid[k] = pick(psf_v[aligned(r, c)], r, c, j, number, grid[k])
            return carry

        lax.fori_loop(0, found, fill, 0)
        couple[...] = jnp.sum(grid[...], axis=1)

    @pl.when(jnp.logical_not(is_root))
    def _():
        couple[...] = jnp.zeros_like(couple)


def make_tables(positions, residual, psf):
    f32 = jnp.float32
    anywhere, vmem = pl.BlockSpec(memory_space=pl.ANY), pl.BlockSpec(memory_space=pltpu.VMEM)
    return pl.pallas_call(
        table_kernel,
        out_shape=(jax.ShapeDtypeStruct((8, LANES), f32), jax.ShapeDtypeStruct((positions.shape[1], LANES), f32)),
        in_specs=[pl.BlockSpec(memory_space=pltpu.SMEM), anywhere, anywhere],
        out_specs=(vmem, vmem),
        scratch_shapes=[
            pltpu.VMEM((positions.shape[1], 8, LANES), f32), pltpu.VMEM(psf.shape[1:], f32),
            pltpu.VMEM((positions.shape[1], 8, LANES), f32), pltpu.SMEM((positions.shape[1] ** 2,), jnp.int32),
            pltpu.SemaphoreType.DMA, pltpu.SemaphoreType.DMA((positions.shape[1],)),
        ],
        name="make_tables",
    )(positions, residual, psf)


def gather_kernel(nchan, nrows, psf, start_own, couple_own, win, amps_out, psf_v, couple_in, start_in, tables, amps_v,
                  load_sem, keep_sem, send_sem, recv_sem, pass_sem, start_send, start_recv, couple_sem, table_send, table_recv, amp_send, amp_recv):
    chan, row = lax.axis_index("chan"), lax.axis_index("rows")
    chip, core = row // 2, row % 2
    partner = row + 1 - 2 * core
    nchips = nrows // 2
    slab = psf.shape[1] // nrows
    unit = 2 * slab
    low, high = nchips - 1, nchips
    steps = couple_own.shape[0]
    lane = lax.broadcasted_iota(jnp.int32, (1, LANES), 1)

    load = pltpu.make_async_copy(psf.at[0], psf_v, load_sem)
    is_low, is_high = row == low, row == high
    is_root = jnp.logical_or(is_low, is_high)

    @pl.when(is_root)
    def _():
        load.start()

    barrier = pltpu.get_barrier_semaphore()
    for step in range(1, nrows):
        pl.semaphore_signal(barrier, inc=1, device_id=(chan, (row + step) % nrows), device_id_type=MESH)
    for step in range(1, nchan):
        pl.semaphore_signal(barrier, inc=1, device_id=((chan + step) % nchan, row), device_id_type=MESH)
    pl.semaphore_wait(barrier, nrows + nchan - 2)

    def piece(to_row, z, m, h, index):
        return pltpu.make_async_remote_copy(
            src_ref=psf.at[0, pl.ds(index, slab)], dst_ref=win.at[pl.ds(m * unit + h * slab, slab)],
            send_sem=send_sem.at[z, m, h], recv_sem=recv_sem.at[m, h], device_id=(chan, to_row), device_id_type=MESH)

    def pieces(root, zs):
        out = []
        for m in range(nchips + 1):
            for z in zs:
                if (z + m < nchips) != (root == low):
                    continue
                for h in range(2):
                    to_row = root ^ 1 if z == root // 2 else 2 * z + h
                    out.append(piece(to_row, z, m, h, ((z + m) % nchips) * unit + h * slab))
        return out

    away = {low: [z for z in range(nchips) if z < low // 2], high: [z for z in range(nchips) if z > high // 2]}
    back = {low: [z for z in range(nchips) if z >= low // 2], high: [z for z in range(nchips) if z <= high // 2]}

    def kept(root):
        z = root // 2
        out = []
        for m in range(nchips + 1):
            if (z + m < nchips) == (root == low):
                out.append(pltpu.make_async_copy(psf_v.at[pl.ds(((z + m) % nchips) * unit, unit)], win.at[pl.ds(m * unit, unit)], keep_sem.at[m]))
        return out

    for root in (low, high):
        @pl.when(row == root)
        def _(root=root):
            for copy in pieces(root, away[root]):
                copy.start()

    def start_copy(source):
        return pltpu.make_async_remote_copy(
            src_ref=start_own, dst_ref=start_in.at[source], send_sem=start_send, recv_sem=start_recv.at[source],
            device_id=(chan, low), device_id_type=MESH)

    @pl.when(jnp.logical_not(is_low))
    def _():
        start_copy(row).start()

    couple_copy = pltpu.make_async_remote_copy(
        src_ref=couple_own, dst_ref=couple_in, send_sem=couple_sem.at[0], recv_sem=couple_sem.at[1],
        device_id=(chan, low), device_id_type=MESH)

    @pl.when(is_high)
    def _():
        couple_copy.start()

    for root in (low, high):
        @pl.when(row == root)
        def _(root=root):
            for copy in pieces(root, back[root]):
                copy.start()
            load.wait()
            for copy in kept(root):
                copy.start()

    def amp_copy(step):
        return pltpu.make_async_remote_copy(
            src_ref=amps_v, dst_ref=amps_v, send_sem=amp_send.at[step], recv_sem=amp_recv,
            device_id=(chan, (low + step) % nrows), device_id_type=MESH)

    def table_copy(peer, owner):
        return pltpu.make_async_remote_copy(
            src_ref=tables.at[owner], dst_ref=tables.at[owner], send_sem=table_send.at[peer], recv_sem=table_recv.at[owner],
            device_id=(peer, low), device_id_type=MESH)

    def relay(m):
        block = at(m * unit + core * slab, slab)
        return pltpu.make_async_remote_copy(
            src_ref=win.at[block], dst_ref=win.at[block], send_sem=pass_sem.at[m], recv_sem=recv_sem.at[m, core],
            device_id=(chan, partner), device_id_type=MESH)

    def arrival(m, h):
        return pltpu.make_async_remote_copy(
            src_ref=win.at[at(m * unit + h * slab, slab)], dst_ref=win.at[at(m * unit + h * slab, slab)],
            send_sem=pass_sem.at[m], recv_sem=recv_sem.at[m, h], device_id=(chan, partner), device_id_type=MESH)

    @pl.when(is_low)
    def _():
        total = start_own[...]
        for step in range(1, nrows):
            source = (low + step) % nrows
            start_copy(source).wait_recv()
            total = total + start_in[source]
        couple_copy.wait_recv()
        tables[chan, pl.ds(0, steps), :] = couple_own[...] + couple_in[...]
        tables[chan, pl.ds(steps, 8), :] = jnp.broadcast_to(jnp.sum(total, axis=0, keepdims=True), total.shape)
        for step in range(1, nchan):
            table_copy((chan + step) % nchan, chan).start()
        for step in range(1, nchan):
            table_copy((chan + step) % nchan, (chan + step) % nchan).wait_recv()
        start = jnp.concatenate([tables[c, pl.ds(steps, 1), :] for c in range(nchan)], axis=0)

        def solve(k, amps):
            couple = jnp.concatenate([tables[c, pl.ds(k, 1), :] for c in range(nchan)], axis=0)
            value = jnp.sum(jnp.where(lane == k, start, 0.0) - amps * couple, axis=1, keepdims=True)
            amp = 0.25 * (value + jnp.sum(value, axis=0, keepdims=True) / nchan)
            return jnp.where(lane == k, amp, amps)

        amps = lax.fori_loop(0, steps, solve, jnp.zeros((nchan, LANES), jnp.float32))
        amps_v[pl.ds(0, nchan), :] = amps
        amps_v[pl.ds(nchan, 8 - nchan), :] = jnp.zeros((8 - nchan, LANES), jnp.float32)
        for step in range(1, nrows):
            amp_copy(step).start()

    for m in range(nchips + 1):
        root = jnp.where(chip + m < nchips, low, high)
        relays = jnp.logical_and(row != root, partner != root)

        @pl.when(relays)
        def _(m=m):
            arrival(m, core).wait_recv()
            relay(m).start()

    for m in range(nchips + 1):
        root = jnp.where(chip + m < nchips, low, high)

        @pl.when(jnp.logical_and(row != root, partner != root))
        def _(m=m):
            arrival(m, 1 - core).wait_recv()
            relay(m).wait_send()

        @pl.when(partner == root)
        def _(m=m):
            arrival(m, 0).wait_recv()
            arrival(m, 1).wait_recv()

    for root in (low, high):
        @pl.when(row == root)
        def _(root=root):
            for copy in kept(root):
                copy.wait()
            for copy in pieces(root, away[root]) + pieces(root, back[root]):
                copy.wait_send()

    @pl.when(is_high)
    def _():
        couple_copy.wait_send()

    @pl.when(is_low)
    def _():
        for step in range(1, nchan):
            table_copy((chan + step) % nchan, chan).wait_send()
        for step in range(1, nrows):
            amp_copy(step).wait_send()

    @pl.when(jnp.logical_not(is_low))
    def _():
        start_copy(row).wait_send()
        amp_copy(1).wait_recv()

    amps_out[...] = amps_v[...]


def gather_patch(nchan, nrows, psf, start, couple):
    shard, patch = psf.shape[1:]
    steps, slab = couple.shape[0], shard // nrows
    nchips = nrows // 2
    rows = slab * (nrows + 2)
    dma, f32 = pltpu.SemaphoreType.DMA, jnp.float32
    anywhere = pl.BlockSpec(memory_space=pl.ANY)
    return pl.pallas_call(
        functools.partial(gather_kernel, nchan, nrows),
        out_shape=(jax.ShapeDtypeStruct((rows, patch), f32), jax.ShapeDtypeStruct((8, LANES), f32)),
        in_specs=[anywhere, pl.BlockSpec(memory_space=pltpu.VMEM), pl.BlockSpec(memory_space=pltpu.VMEM)],
        out_specs=(anywhere, pl.BlockSpec(memory_space=pltpu.VMEM)),
        scratch_shapes=[
            pltpu.VMEM((shard, patch), f32), pltpu.VMEM((steps, LANES), f32), pltpu.VMEM((nrows, 8, LANES), f32),
            pltpu.VMEM((nchan, steps + 8, LANES), f32), pltpu.VMEM((8, LANES), f32),
            dma, dma((nchips + 1,)), dma((nchips, nchips + 1, 2)), dma((nchips + 1, 2)), dma((nchips + 1,)),
            dma, dma((nrows,)), dma((2,)), dma((nchan,)), dma((nchan,)), dma((nrows,)), dma,
        ],
        compiler_params=pltpu.CompilerParams(collective_id=0, has_side_effects=True),
        name="gather_patch",
    )(psf, start, couple)


def apply_kernel(pos, amps, res, win, out, image, patch_v, sems):
    chan, row = lax.axis_index("chan"), lax.axis_index("rows")
    nrows = lax.axis_size("rows")
    slab, ncols = res.shape[1], res.shape[2]
    rows, patch = win.shape
    chunks = patch // LANES
    tiles = slab // 8
    loads = [pltpu.make_async_copy(win.at[:, pl.ds(c * LANES, LANES)], patch_v.at[c], sems.at[c]) for c in range(chunks)]

    def band(t):
        return pltpu.make_async_copy(res.at[0, pl.ds(8 * t, 8)], image.at[pl.ds(8 * t, 8), pl.ds(0, ncols)], sems.at[chunks + t])

    def done(t):
        return pltpu.make_async_copy(image.at[pl.ds(8 * t, 8), pl.ds(0, ncols)], out.at[0, pl.ds(8 * t, 8)], sems.at[chunks + tiles + t])

    band(0).start()
    for copy in loads:
        copy.start()
    for t in range(1, tiles):
        band(t).start()
    for copy in loads:
        copy.wait()
    lane = lax.broadcasted_iota(jnp.int32, (8, LANES), 1)
    top = (row % 2) * slab + slab * nrows

    zero = jnp.zeros((8, LANES), jnp.float32)
    for pair in range(tiles // 2):
        mine = (2 * pair, 2 * pair + 1)
        for t in mine:
            band(t).wait()

        def step(k, carry, mine=mine):
            amp = amps[chan, k]
            begin = top - pos[0, k]
            left = pos[1, k] - patch // 2
            shift = left & (LANES - 1)
            span = pl.ds(pl.multiple_of(left - shift, LANES), patch + LANES)
            keep = lane < shift
            for t in mine:
                moved = [zero] + [pltpu.roll(patch_v[c, pl.ds(begin + 8 * t, 8), :] * amp, shift, 1) for c in range(chunks)] + [zero]
                change = jnp.concatenate([jnp.where(keep, moved[c], moved[c + 1]) for c in range(chunks + 1)], axis=1)
                image[pl.ds(8 * t, 8), span] = image[pl.ds(8 * t, 8), span] - change
            return carry

        lax.fori_loop(0, pos.shape[1], step, 0)
        for t in mine:
            done(t).start()
    for t in range(tiles):
        done(t).wait()


def apply_peaks(positions, amps, residual, win):
    slab, ncols = residual.shape[1:]
    rows, patch = win.shape
    chunks = patch // LANES
    anywhere, scalars = pl.BlockSpec(memory_space=pl.ANY), pl.BlockSpec(memory_space=pltpu.SMEM)
    return pl.pallas_call(
        apply_kernel,
        out_shape=jax.ShapeDtypeStruct(residual.shape, jnp.float32),
        in_specs=[scalars, scalars, anywhere, anywhere],
        out_specs=anywhere,
        scratch_shapes=[
            pltpu.VMEM((slab, ncols + LANES), jnp.float32), pltpu.VMEM((chunks, rows, LANES), jnp.float32),
            pltpu.SemaphoreType.DMA((chunks + slab // 4,)),
        ],
        name="apply_peaks",
    )(positions, amps, residual, win)


def sum_kernel(nchan, nrows, image, out, total_out, own, near, first_far, first_own, passed, second, squares,
               load_sem, far_send, far_recv, own_send, own_recv, pass_send, pass_recv, square_send, square_recv):
    chan, row = lax.axis_index("chan"), lax.axis_index("rows")
    me = row * nchan + chan
    slab, ncols = image.shape[1], image.shape[2]
    cols = ncols // nchan
    part = slab // 2
    width = cols // PIECES
    bits = ((1, 2), (2, 1))

    def block(c):
        return pl.ds(pl.multiple_of(c * cols, LANES), cols)

    def flip(bit):
        if bit == 1:
            return chan + 1 - 2 * (chan % 2)
        return (chan + 2) % 4

    diagonal = 3 - chan
    loads = [pltpu.make_async_copy(image.at[0, :, block(chan)], own, load_sem.at[0])]
    for p in range(2):
        loads.append(pltpu.make_async_copy(image.at[0, pl.ds(p * part, part), block(flip(bits[p][1]))], near.at[p], load_sem.at[1 + p]))
    for copy in loads:
        copy.start()

    barrier = pltpu.get_barrier_semaphore()
    for step in range(1, nrows * nchan):
        other = (me + step) % (nrows * nchan)
        pl.semaphore_signal(barrier, inc=1, device_id=(other % nchan, other // nchan), device_id_type=MESH)
    pl.semaphore_wait(barrier, nrows * nchan - 1)

    def send(p, g, source, dest, send_sem, recv_sem, to):
        return pltpu.make_async_remote_copy(
            src_ref=source, dst_ref=dest.at[p, :, pl.ds(g * width, width)], send_sem=send_sem.at[p, g], recv_sem=recv_sem.at[p, g],
            device_id=(to, row), device_id_type=MESH)

    def tile(p, g, c):
        return image.at[0, pl.ds(p * part, part), pl.ds(pl.multiple_of(c * cols + g * width, LANES), width)]

    def far(p, g):
        return send(p, g, tile(p, g, diagonal), first_far, far_send, far_recv, flip(bits[p][0]))

    def mine(p, g):
        return send(p, g, tile(p, g, flip(bits[p][0])), first_own, own_send, own_recv, flip(bits[p][0]))

    def onward(p, g):
        return send(p, g, passed.at[p, :, pl.ds(g * width, width)], second, pass_send, pass_recv, flip(bits[p][1]))

    for g in range(PIECES):
        for p in range(2):
            far(p, g).start()
    for g in range(PIECES):
        for p in range(2):
            mine(p, g).start()
    for copy in loads:
        copy.wait()
    for g in range(PIECES):
        for p in range(2):
            span = pl.ds(g * width, width)
            far(p, g).wait_recv()
            passed[p, :, span] = near[p, :, span] + first_far[p, :, span]
            onward(p, g).start()
    for g in range(PIECES):
        for p in range(2):
            span = pl.ds(g * width, width)
            mine(p, g).wait_recv()
            rows = pl.ds(p * part, part)
            own[rows, span] = own[rows, span] + first_own[p, :, span]
    total = jnp.zeros((8, LANES), jnp.float32)
    for g in range(PIECES):
        for p in range(2):
            span = pl.ds(g * width, width)
            onward(p, g).wait_recv()
            rows = pl.ds(p * part, part)
            value = own[rows, span] + second[p, :, span]
            own[rows, span] = value
            square = value * value
            for t in range(part // 8):
                for c in range(width // LANES):
                    total = total + square[8 * t:8 * t + 8, c * LANES:(c + 1) * LANES]
    squares[pl.ds(me, 1), :] = jnp.sum(total, axis=0, keepdims=True)

    def spread(step):
        other = (me + step) % (nrows * nchan)
        return pltpu.make_async_remote_copy(
            src_ref=squares.at[pl.ds(me, 1)], dst_ref=squares.at[pl.ds(me, 1)], send_sem=square_send.at[step], recv_sem=square_recv.at[step],
            device_id=(other % nchan, other // nchan), device_id_type=MESH)

    def arrived(step):
        other = (me + nrows * nchan - step) % (nrows * nchan)
        return pltpu.make_async_remote_copy(
            src_ref=squares.at[pl.ds(other, 1)], dst_ref=squares.at[pl.ds(other, 1)], send_sem=square_send.at[step], recv_sem=square_recv.at[step],
            device_id=(other % nchan, other // nchan), device_id_type=MESH)

    for step in range(1, nrows * nchan):
        spread(step).start()
    keep = pltpu.make_async_copy(own, out, load_sem.at[0])
    keep.start()
    for step in range(1, nrows * nchan):
        arrived(step).wait_recv()
    everything = jnp.sum(jnp.sum(squares[...], axis=0, keepdims=True), axis=1, keepdims=True)
    total_out[...] = jnp.broadcast_to(everything, total_out.shape)
    keep.wait()
    for step in range(1, nrows * nchan):
        spread(step).wait_send()
    for g in range(PIECES):
        for p in range(2):
            far(p, g).wait_send()
            mine(p, g).wait_send()
            onward(p, g).wait_send()


def sum_channels(nchan, nrows, image):
    slab, ncols = image.shape[1:]
    cols, part = ncols // nchan, slab // 2
    dma, f32 = pltpu.SemaphoreType.DMA, jnp.float32
    halves = pltpu.VMEM((2, part, cols), f32)
    parts, total = pl.pallas_call(
        functools.partial(sum_kernel, nchan, nrows),
        out_shape=(jax.ShapeDtypeStruct((slab, cols), f32), jax.ShapeDtypeStruct((8, LANES), f32)),
        in_specs=[pl.BlockSpec(memory_space=pl.ANY)],
        out_specs=(pl.BlockSpec(memory_space=pl.ANY), pl.BlockSpec(memory_space=pltpu.VMEM)),
        scratch_shapes=[pltpu.VMEM((slab, cols), f32)] + [halves] * 5 + [pltpu.VMEM((nrows * nchan, LANES), f32), dma((3,))]
        + [dma((2, PIECES))] * 6 + [dma((nrows * nchan,))] * 2,
        compiler_params=pltpu.CompilerParams(collective_id=1, has_side_effects=True),
        name="sum_channels",
    )(image)
    return parts * lax.rsqrt(total[0, 0] / (slab * nrows * ncols) + 1e-06)


def on_device(residual, psf, positions):
    nchan, nrows = lax.axis_size("chan"), lax.axis_size("rows")
    slab, ncols = residual.shape[1:]
    shard, patch = psf.shape[1:]
    central = nrows % 2 == 0 and slab * nrows == shard and 2 * shard * (nrows // 2) == patch
    powers = shard & (shard - 1) == 0 and patch & (patch - 1) == 0
    if not (central and powers and nchan == 4 and slab % 16 == 0 and positions.shape[0] % 8 == 0 and positions.shape[0] <= LANES):
        return on_any_device(residual, psf, positions)
    positions = positions.T
    start, couple = make_tables(positions, residual, psf)
    win, amps = gather_patch(nchan, nrows, psf, start, couple)
    image = apply_peaks(positions, amps, residual, win)
    return (image, sum_channels(nchan, nrows, image))


def on_any_device(residual, psf, positions):
    chan_id = lax.axis_index("chan")
    nchan = lax.axis_size("chan")
    row_id = lax.axis_index("rows")
    nrows = lax.axis_size("rows")
    slab = residual.shape[1]
    ncols = residual.shape[2]
    own_psf = psf[0]
    shard_rows = own_psf.shape[0]
    patch = own_psf.shape[1]
    half = patch // 2
    first = row_id * slab
    chan_hot = (jnp.arange(nchan) == chan_id).astype(jnp.float32)
    full_psf = lax.all_gather(own_psf, "rows", axis=0, tiled=True)
    padded_psf = jnp.pad(full_psf, ((slab, slab), (0, 0)))
    zero = jnp.int32(0)

    def subtract(image, row, col, amount):
        offset = first - row + half
        touches = jnp.logical_and(offset > -slab, offset < patch)
        start = jnp.clip(offset + slab, 0, patch + slab)
        psf_rows = lax.dynamic_slice(padded_psf, (start, zero), (slab, patch))
        window = lax.dynamic_slice(image, (zero, col - half), (slab, patch))
        scale = jnp.where(touches, amount, 0.0)
        return lax.dynamic_update_slice(image, window - scale * psf_rows, (zero, col - half))

    image = residual[0]
    peak_rows = positions[:, 0]
    peak_cols = positions[:, 1]
    inside = jnp.logical_and(peak_rows >= first, peak_rows < first + slab)
    local_rows = jnp.clip(peak_rows - first, 0, slab - 1)
    start_values = jnp.where(inside, image[local_rows, peak_cols], 0.0)
    row_offset = peak_rows[:, None] - peak_rows[None, :] + half - row_id * shard_rows
    col_offset = peak_cols[:, None] - peak_cols[None, :] + half
    owned = (row_offset >= 0) & (row_offset < shard_rows) & (col_offset >= 0) & (col_offset < patch)
    couple = own_psf[jnp.clip(row_offset, 0, shard_rows - 1), jnp.clip(col_offset, 0, patch - 1)]
    couple = jnp.where(owned, couple, 0.0)
    start_table, couple_table = lax.psum(
        (chan_hot[:, None] * start_values[None, :], chan_hot[:, None, None] * couple[None, :, :]),
        ("chan", "rows"),
    )

    def solve(k, amps):
        taken = jnp.sum(amps * lax.dynamic_index_in_dim(couple_table, k, 1, False), axis=1)
        value = lax.dynamic_index_in_dim(start_table, k, 1, False) - taken
        amp = 0.25 * (value + jnp.sum(value) / nchan)
        return lax.dynamic_update_index_in_dim(amps, amp, k, 1)

    amps = lax.fori_loop(0, STEPS, solve, jnp.zeros((nchan, STEPS), jnp.float32))
    own_amps = jnp.sum(chan_hot[:, None] * amps, axis=0)

    def apply(k, image):
        return subtract(image, positions[k, 0], positions[k, 1], own_amps[k])

    image = lax.fori_loop(0, STEPS, apply, image)
    count = slab * nrows * ncols
    parts = lax.psum_scatter(image, "chan", scatter_dimension=1, tiled=True)
    total = lax.psum(jnp.sum(parts * parts), ("chan", "rows"))
    normalized = parts * lax.rsqrt(total / count + 1e-06)
    return (image[None], normalized)


def solution(mesh):
    return jax.shard_map(
        on_device,
        mesh=mesh,
        in_specs=(P("chan", "rows", None), P("chan", "rows", None), P()),
        out_specs=(P("chan", "rows", None), P("rows", "chan")),
        check_vma=False,
    )
```

```python
import functools

import jax
import jax.numpy as jnp
from jax import lax
from jax.experimental import pallas as pl
from jax.experimental.pallas import tpu as pltpu
from jax.sharding import PartitionSpec as P

STEPS = 32
LANES = 128
PIECES = 4
MESH = pl.DeviceIdType.MESH


def at(start, size):
    return pl.ds(pl.multiple_of(start, 8), size)


def aligned(row, col):
    return (pl.ds(pl.multiple_of((row >> 3) << 3, 8), 8), pl.ds(pl.multiple_of((col >> 7) << 7, LANES), LANES))


def pick(tile, row, col, lane_to, number, acc):
    moved = pltpu.roll(tile, (lane_to - col) & (LANES - 1), 1)
    return jnp.where(number == (row & 7) * LANES + lane_to, moved, acc)


def table_kernel(pos, res, psf, start, couple, tiles, psf_v, grid, pairs, load_sem, sems):
    row, nrows = lax.axis_index("rows"), lax.axis_size("rows")
    slab, steps = res.shape[1], pos.shape[1]
    shard, patch = psf.shape[1:]
    half = patch // 2
    first = row * slab
    is_root = jnp.logical_or(row == nrows // 2 - 1, row == nrows // 2)
    load = pltpu.make_async_copy(psf.at[0], psf_v, load_sem)

    @pl.when(is_root)
    def _():
        load.start()

    loads = []
    for k in range(steps):
        rows, cols = aligned(jnp.clip(pos[0, k] - first, 0, slab - 1), pos[1, k])
        loads.append(pltpu.make_async_copy(res.at[0, rows, cols], tiles.at[k], sems.at[k]))
    for copy in loads:
        copy.start()
    lane = lax.broadcasted_iota(jnp.int32, (1, LANES), 1)
    number = lax.broadcasted_iota(jnp.int32, (8, LANES), 0) * LANES + lax.broadcasted_iota(jnp.int32, (8, LANES), 1)
    peak_rows, peak_cols = jnp.zeros((1, LANES), jnp.int32), jnp.zeros((1, LANES), jnp.int32)
    for k in range(steps):
        peak_rows = jnp.where(lane == k, pos[0, k], peak_rows)
        peak_cols = jnp.where(lane == k, pos[1, k], peak_cols)
    for copy in loads:
        copy.wait()
    acc = jnp.zeros((8, LANES), jnp.float32)
    for k in range(steps):
        acc = pick(tiles[k], pos[0, k] - first, pos[1, k], k, number, acc)
    inside = (peak_rows >= first) & (peak_rows < first + slab) & (lane < steps)
    start[...] = jnp.where(inside, acc, 0.0)

    @pl.when(is_root)
    def _():
        grid[...] = jnp.zeros_like(grid)
        low = row * shard - half

        def listed(k, found):
            rk, qk = pos[0, k] - low, pos[1, k] + half

            def test(g, found):
                for i in range(8):
                    j = g * 8 + i
                    r, c = rk - pos[0, j], qk - pos[1, j]
                    owned = (r >= 0) & (r < shard) & (c >= 0) & (c < patch) & (j < k)
                    pairs[found] = k * steps + j
                    found = found + owned.astype(jnp.int32)
                return found

            return lax.fori_loop(0, (k + 7) >> 3, test, found)

        found = lax.fori_loop(0, steps, listed, jnp.int32(0))
        load.wait()

        def fill(n, carry):
            k, j = pairs[n] // steps, pairs[n] % steps
            r, c = pos[0, k] - low - pos[0, j], pos[1, k] + half - pos[1, j]
            grid[k] = pick(psf_v[aligned(r, c)], r, c, j, number, grid[k])
            return carry

        lax.fori_loop(0, found, fill, 0)
        couple[...] = jnp.sum(grid[...], axis=1)

    @pl.when(jnp.logical_not(is_root))
    def _():
        couple[...] = jnp.zeros_like(couple)


def make_tables(positions, residual, psf):
    f32 = jnp.float32
    anywhere, vmem = pl.BlockSpec(memory_space=pl.ANY), pl.BlockSpec(memory_space=pltpu.VMEM)
    return pl.pallas_call(
        table_kernel,
        out_shape=(jax.ShapeDtypeStruct((8, LANES), f32), jax.ShapeDtypeStruct((positions.shape[1], LANES), f32)),
        in_specs=[pl.BlockSpec(memory_space=pltpu.SMEM), anywhere, anywhere],
        out_specs=(vmem, vmem),
        scratch_shapes=[
            pltpu.VMEM((positions.shape[1], 8, LANES), f32), pltpu.VMEM(psf.shape[1:], f32),
            pltpu.VMEM((positions.shape[1], 8, LANES), f32), pltpu.SMEM((positions.shape[1] ** 2,), jnp.int32),
            pltpu.SemaphoreType.DMA, pltpu.SemaphoreType.DMA((positions.shape[1],)),
        ],
        name="make_tables",
    )(positions, residual, psf)


def gather_kernel(nchan, nrows, psf, start_own, couple_own, win, amps_out, psf_v, couple_in, start_in, tables, amps_v,
                  load_sem, keep_sem, send_sem, recv_sem, pass_sem, start_send, start_recv, couple_sem, table_send, table_recv, amp_send, amp_recv):
    chan, row = lax.axis_index("chan"), lax.axis_index("rows")
    chip, core = row // 2, row % 2
    partner = row + 1 - 2 * core
    nchips = nrows // 2
    slab = psf.shape[1] // nrows
    unit = 2 * slab
    low, high = nchips - 1, nchips
    steps = couple_own.shape[0]
    lane = lax.broadcasted_iota(jnp.int32, (1, LANES), 1)

    load = pltpu.make_async_copy(psf.at[0], psf_v, load_sem)
    is_low, is_high = row == low, row == high
    is_root = jnp.logical_or(is_low, is_high)

    @pl.when(is_root)
    def _():
        load.start()

    barrier = pltpu.get_barrier_semaphore()
    for step in range(1, nrows):
        pl.semaphore_signal(barrier, inc=1, device_id=(chan, (row + step) % nrows), device_id_type=MESH)
    for step in range(1, nchan):
        pl.semaphore_signal(barrier, inc=1, device_id=((chan + step) % nchan, row), device_id_type=MESH)
    pl.semaphore_wait(barrier, nrows + nchan - 2)

    def piece(to_row, z, m, h, index):
        return pltpu.make_async_remote_copy(
            src_ref=psf.at[0, pl.ds(index, slab)], dst_ref=win.at[pl.ds(m * unit + h * slab, slab)],
            send_sem=send_sem.at[z, m, h], recv_sem=recv_sem.at[m, h], device_id=(chan, to_row), device_id_type=MESH)

    def pieces(root, zs):
        out = []
        for m in range(nchips + 1):
            for z in zs:
                if (z + m < nchips) != (root == low):
                    continue
                for h in range(2):
                    to_row = root ^ 1 if z == root // 2 else 2 * z + h
                    out.append(piece(to_row, z, m, h, ((z + m) % nchips) * unit + h * slab))
        return out

    away = {low: [z for z in range(nchips) if z < low // 2], high: [z for z in range(nchips) if z > high // 2]}
    back = {low: [z for z in range(nchips) if z >= low // 2], high: [z for z in range(nchips) if z <= high // 2]}

    def kept(root):
        z = root // 2
        out = []
        for m in range(nchips + 1):
            if (z + m < nchips) == (root == low):
                out.append(pltpu.make_async_copy(psf_v.at[pl.ds(((z + m) % nchips) * unit, unit)], win.at[pl.ds(m * unit, unit)], keep_sem.at[m]))
        return out

    for root in (low, high):
        @pl.when(row == root)
        def _(root=root):
            for copy in pieces(root, away[root]):
                copy.start()

    def start_copy(source):
        return pltpu.make_async_remote_copy(
            src_ref=start_own, dst_ref=start_in.at[source], send_sem=start_send, recv_sem=start_recv.at[source],
            device_id=(chan, low), device_id_type=MESH)

    @pl.when(jnp.logical_not(is_low))
    def _():
        start_copy(row).start()

    couple_copy = pltpu.make_async_remote_copy(
        src_ref=couple_own, dst_ref=couple_in, send_sem=couple_sem.at[0], recv_sem=couple_sem.at[1],
        device_id=(chan, low), device_id_type=MESH)

    @pl.when(is_high)
    def _():
        couple_copy.start()

    for root in (low, high):
        @pl.when(row == root)
        def _(root=root):
            for copy in pieces(root, back[root]):
                copy.start()
            load.wait()
            for copy in kept(root):
                copy.start()

    def amp_copy(step):
        return pltpu.make_async_remote_copy(
            src_ref=amps_v, dst_ref=amps_v, send_sem=amp_send.at[step], recv_sem=amp_recv,
            device_id=(chan, (low + step) % nrows), device_id_type=MESH)

    def table_copy(peer, owner):
        return pltpu.make_async_remote_copy(
            src_ref=tables.at[owner], dst_ref=tables.at[owner], send_sem=table_send.at[peer], recv_sem=table_recv.at[owner],
            device_id=(peer, low), device_id_type=MESH)

    def relay(m):
        block = at(m * unit + core * slab, slab)
        return pltpu.make_async_remote_copy(
            src_ref=win.at[block], dst_ref=win.at[block], send_sem=pass_sem.at[m], recv_sem=recv_sem.at[m, core],
            device_id=(chan, partner), device_id_type=MESH)

    def arrival(m, h):
        return pltpu.make_async_remote_copy(
            src_ref=win.at[at(m * unit + h * slab, slab)], dst_ref=win.at[at(m * unit + h * slab, slab)],
            send_sem=pass_sem.at[m], recv_sem=recv_sem.at[m, h], device_id=(chan, partner), device_id_type=MESH)

    @pl.when(is_low)
    def _():
        total = start_own[...]
        for step in range(1, nrows):
            source = (low + step) % nrows
            start_copy(source).wait_recv()
            total = total + start_in[source]
        couple_copy.wait_recv()
        tables[chan, pl.ds(0, steps), :] = couple_own[...] + couple_in[...]
        tables[chan, pl.ds(steps, 8), :] = jnp.broadcast_to(jnp.sum(total, axis=0, keepdims=True), total.shape)
        for step in range(1, nchan):
            table_copy((chan + step) % nchan, chan).start()
        for step in range(1, nchan):
            table_copy((chan + step) % nchan, (chan + step) % nchan).wait_recv()
        start = jnp.concatenate([tables[c, pl.ds(steps, 1), :] for c in range(nchan)], axis=0)

        def solve(k, amps):
            couple = jnp.concatenate([tables[c, pl.ds(k, 1), :] for c in range(nchan)], axis=0)
            value = jnp.sum(jnp.where(lane == k, start, 0.0) - amps * couple, axis=1, keepdims=True)
            amp = 0.25 * (value + jnp.sum(value, axis=0, keepdims=True) / nchan)
            return jnp.where(lane == k, amp, amps)

        amps = lax.fori_loop(0, steps, solve, jnp.zeros((nchan, LANES), jnp.float32))
        amps_v[pl.ds(0, nchan), :] = amps
        amps_v[pl.ds(nchan, 8 - nchan), :] = jnp.zeros((8 - nchan, LANES), jnp.float32)
        for step in range(1, nrows):
            amp_copy(step).start()

    for m in range(nchips + 1):
        root = jnp.where(chip + m < nchips, low, high)
        relays = jnp.logical_and(row != root, partner != root)

        @pl.when(relays)
        def _(m=m):
            arrival(m, core).wait_recv()
            relay(m).start()

    for m in range(nchips + 1):
        root = jnp.where(chip + m < nchips, low, high)

        @pl.when(jnp.logical_and(row != root, partner != root))
        def _(m=m):
            arrival(m, 1 - core).wait_recv()
            relay(m).wait_send()

        @pl.when(partner == root)
        def _(m=m):
            arrival(m, 0).wait_recv()
            arrival(m, 1).wait_recv()

    for root in (low, high):
        @pl.when(row == root)
        def _(root=root):
            for copy in kept(root):
                copy.wait()
            for copy in pieces(root, away[root]) + pieces(root, back[root]):
                copy.wait_send()

    @pl.when(is_high)
    def _():
        couple_copy.wait_send()

    @pl.when(is_low)
    def _():
        for step in range(1, nchan):
            table_copy((chan + step) % nchan, chan).wait_send()
        for step in range(1, nrows):
            amp_copy(step).wait_send()

    @pl.when(jnp.logical_not(is_low))
    def _():
        start_copy(row).wait_send()
        amp_copy(1).wait_recv()

    amps_out[...] = amps_v[...]


def gather_patch(nchan, nrows, psf, start, couple):
    shard, patch = psf.shape[1:]
    steps, slab = couple.shape[0], shard // nrows
    nchips = nrows // 2
    rows = slab * (nrows + 2)
    dma, f32 = pltpu.SemaphoreType.DMA, jnp.float32
    anywhere = pl.BlockSpec(memory_space=pl.ANY)
    return pl.pallas_call(
        functools.partial(gather_kernel, nchan, nrows),
        out_shape=(jax.ShapeDtypeStruct((rows, patch), f32), jax.ShapeDtypeStruct((8, LANES), f32)),
        in_specs=[anywhere, pl.BlockSpec(memory_space=pltpu.VMEM), pl.BlockSpec(memory_space=pltpu.VMEM)],
        out_specs=(anywhere, pl.BlockSpec(memory_space=pltpu.VMEM)),
        scratch_shapes=[
            pltpu.VMEM((shard, patch), f32), pltpu.VMEM((steps, LANES), f32), pltpu.VMEM((nrows, 8, LANES), f32),
            pltpu.VMEM((nchan, steps + 8, LANES), f32), pltpu.VMEM((8, LANES), f32),
            dma, dma((nchips + 1,)), dma((nchips, nchips + 1, 2)), dma((nchips + 1, 2)), dma((nchips + 1,)),
            dma, dma((nrows,)), dma((2,)), dma((nchan,)), dma((nchan,)), dma((nrows,)), dma,
        ],
        compiler_params=pltpu.CompilerParams(collective_id=0, has_side_effects=True),
        name="gather_patch",
    )(psf, start, couple)


def apply_kernel(pos, amps, res, win, out, image, patch_v, sems):
    chan, row = lax.axis_index("chan"), lax.axis_index("rows")
    nrows = lax.axis_size("rows")
    slab, ncols = res.shape[1], res.shape[2]
    rows, patch = win.shape
    chunks = patch // LANES
    tiles = slab // 8
    loads = [pltpu.make_async_copy(win.at[:, pl.ds(c * LANES, LANES)], patch_v.at[c], sems.at[c]) for c in range(chunks)]

    def band(t):
        return pltpu.make_async_copy(res.at[0, pl.ds(8 * t, 8)], image.at[pl.ds(8 * t, 8), pl.ds(0, ncols)], sems.at[chunks + t])

    def done(t):
        return pltpu.make_async_copy(image.at[pl.ds(8 * t, 8), pl.ds(0, ncols)], out.at[0, pl.ds(8 * t, 8)], sems.at[chunks + tiles + t])

    band(0).start()
    for copy in loads:
        copy.start()
    for t in range(1, tiles):
        band(t).start()
    for copy in loads:
        copy.wait()
    lane = lax.broadcasted_iota(jnp.int32, (8, LANES), 1)
    top = (row % 2) * slab + slab * nrows

    zero = jnp.zeros((8, LANES), jnp.float32)
    for pair in range(tiles // 2):
        mine = (2 * pair, 2 * pair + 1)
        for t in mine:
            band(t).wait()

        def step(k, carry, mine=mine):
            amp = amps[chan, k]
            begin = top - pos[0, k]
            left = pos[1, k] - patch // 2
            shift = left & (LANES - 1)
            span = pl.ds(pl.multiple_of(left - shift, LANES), patch + LANES)
            keep = lane < shift
            for t in mine:
                moved = [zero] + [pltpu.roll(patch_v[c, pl.ds(begin + 8 * t, 8), :] * amp, shift, 1) for c in range(chunks)] + [zero]
                change = jnp.concatenate([jnp.where(keep, moved[c], moved[c + 1]) for c in range(chunks + 1)], axis=1)
                image[pl.ds(8 * t, 8), span] = image[pl.ds(8 * t, 8), span] - change
            return carry

        lax.fori_loop(0, pos.shape[1], step, 0)
        for t in mine:
            done(t).start()
    for t in range(tiles):
        done(t).wait()


def apply_peaks(positions, amps, residual, win):
    slab, ncols = residual.shape[1:]
    rows, patch = win.shape
    chunks = patch // LANES
    anywhere, scalars = pl.BlockSpec(memory_space=pl.ANY), pl.BlockSpec(memory_space=pltpu.SMEM)
    return pl.pallas_call(
        apply_kernel,
        out_shape=jax.ShapeDtypeStruct(residual.shape, jnp.float32),
        in_specs=[scalars, scalars, anywhere, anywhere],
        out_specs=anywhere,
        scratch_shapes=[
            pltpu.VMEM((slab, ncols + LANES), jnp.float32), pltpu.VMEM((chunks, rows, LANES), jnp.float32),
            pltpu.SemaphoreType.DMA((chunks + slab // 4,)),
        ],
        name="apply_peaks",
    )(positions, amps, residual, win)


def sum_kernel(nchan, nrows, image, out, total_out, own, near, first_far, first_own, passed, second, squares,
               load_sem, far_send, far_recv, own_send, own_recv, pass_send, pass_recv, square_send, square_recv):
    chan, row = lax.axis_index("chan"), lax.axis_index("rows")
    me = row * nchan + chan
    slab, ncols = image.shape[1], image.shape[2]
    cols = ncols // nchan
    part = slab // 2
    width = cols // PIECES
    bits = ((1, 2), (2, 1))

    def block(c):
        return pl.ds(pl.multiple_of(c * cols, LANES), cols)

    def flip(bit):
        if bit == 1:
            return chan + 1 - 2 * (chan % 2)
        return (chan + 2) % 4

    diagonal = 3 - chan
    loads = [pltpu.make_async_copy(image.at[0, :, block(chan)], own, load_sem.at[0])]
    for p in range(2):
        loads.append(pltpu.make_async_copy(image.at[0, pl.ds(p * part, part), block(flip(bits[p][1]))], near.at[p], load_sem.at[1 + p]))
    for copy in loads:
        copy.start()

    barrier = pltpu.get_barrier_semaphore()
    for step in range(1, nrows * nchan):
        other = (me + step) % (nrows * nchan)
        pl.semaphore_signal(barrier, inc=1, device_id=(other % nchan, other // nchan), device_id_type=MESH)
    pl.semaphore_wait(barrier, nrows * nchan - 1)

    def send(p, g, source, dest, send_sem, recv_sem, to):
        return pltpu.make_async_remote_copy(
            src_ref=source, dst_ref=dest.at[p, :, pl.ds(g * width, width)], send_sem=send_sem.at[p, g], recv_sem=recv_sem.at[p, g],
            device_id=(to, row), device_id_type=MESH)

    def tile(p, g, c):
        return image.at[0, pl.ds(p * part, part), pl.ds(pl.multiple_of(c * cols + g * width, LANES), width)]

    def far(p, g):
        return send(p, g, tile(p, g, diagonal), first_far, far_send, far_recv, flip(bits[p][0]))

    def mine(p, g):
        return send(p, g, tile(p, g, flip(bits[p][0])), first_own, own_send, own_recv, flip(bits[p][0]))

    def onward(p, g):
        return send(p, g, passed.at[p, :, pl.ds(g * width, width)], second, pass_send, pass_recv, flip(bits[p][1]))

    for g in range(PIECES):
        for p in range(2):
            far(p, g).start()
    for g in range(PIECES):
        for p in range(2):
            mine(p, g).start()
    for copy in loads:
        copy.wait()
    for g in range(PIECES):
        for p in range(2):
            span = pl.ds(g * width, width)
            far(p, g).wait_recv()
            passed[p, :, span] = near[p, :, span] + first_far[p, :, span]
            onward(p, g).start()
    for g in range(PIECES):
        for p in range(2):
            span = pl.ds(g * width, width)
            mine(p, g).wait_recv()
            rows = pl.ds(p * part, part)
            own[rows, span] = own[rows, span] + first_own[p, :, span]
    total = jnp.zeros((8, LANES), jnp.float32)
    for g in range(PIECES):
        for p in range(2):
            span = pl.ds(g * width, width)
            onward(p, g).wait_recv()
            rows = pl.ds(p * part, part)
            value = own[rows, span] + second[p, :, span]
            own[rows, span] = value
            square = value * value
            for t in range(part // 8):
                for c in range(width // LANES):
                    total = total + square[8 * t:8 * t + 8, c * LANES:(c + 1) * LANES]
    squares[pl.ds(me, 1), :] = jnp.sum(total, axis=0, keepdims=True)

    def spread(step):
        other = (me + step) % (nrows * nchan)
        return pltpu.make_async_remote_copy(
            src_ref=squares.at[pl.ds(me, 1)], dst_ref=squares.at[pl.ds(me, 1)], send_sem=square_send.at[step], recv_sem=square_recv.at[step],
            device_id=(other % nchan, other // nchan), device_id_type=MESH)

    def arrived(step):
        other = (me + nrows * nchan - step) % (nrows * nchan)
        return pltpu.make_async_remote_copy(
            src_ref=squares.at[pl.ds(other, 1)], dst_ref=squares.at[pl.ds(other, 1)], send_sem=square_send.at[step], recv_sem=square_recv.at[step],
            device_id=(other % nchan, other // nchan), device_id_type=MESH)

    for step in range(1, nrows * nchan):
        spread(step).start()
    keep = pltpu.make_async_copy(own, out, load_sem.at[0])
    keep.start()
    for step in range(1, nrows * nchan):
        arrived(step).wait_recv()
    everything = jnp.sum(jnp.sum(squares[...], axis=0, keepdims=True), axis=1, keepdims=True)
    total_out[...] = jnp.broadcast_to(everything, total_out.shape)
    keep.wait()
    for step in range(1, nrows * nchan):
        spread(step).wait_send()
    for g in range(PIECES):
        for p in range(2):
            far(p, g).wait_send()
            mine(p, g).wait_send()
            onward(p, g).wait_send()


def sum_channels(nchan, nrows, image):
    slab, ncols = image.shape[1:]
    cols, part = ncols // nchan, slab // 2
    dma, f32 = pltpu.SemaphoreType.DMA, jnp.float32
    halves = pltpu.VMEM((2, part, cols), f32)
    parts, total = pl.pallas_call(
        functools.partial(sum_kernel, nchan, nrows),
        out_shape=(jax.ShapeDtypeStruct((slab, cols), f32), jax.ShapeDtypeStruct((8, LANES), f32)),
        in_specs=[pl.BlockSpec(memory_space=pl.ANY)],
        out_specs=(pl.BlockSpec(memory_space=pl.ANY), pl.BlockSpec(memory_space=pltpu.VMEM)),
        scratch_shapes=[pltpu.VMEM((slab, cols), f32)] + [halves] * 5 + [pltpu.VMEM((nrows * nchan, LANES), f32), dma((3,))]
        + [dma((2, PIECES))] * 6 + [dma((nrows * nchan,))] * 2,
        compiler_params=pltpu.CompilerParams(collective_id=1, has_side_effects=True),
        name="sum_channels",
    )(image)
    return parts * lax.rsqrt(total[0, 0] / (slab * nrows * ncols) + 1e-06)


def on_device(residual, psf, positions):
    nchan, nrows = lax.axis_size("chan"), lax.axis_size("rows")
    slab, ncols = residual.shape[1:]
    shard, patch = psf.shape[1:]
    central = nrows % 2 == 0 and slab * nrows == shard and 2 * shard * (nrows // 2) == patch
    powers = shard & (shard - 1) == 0 and patch & (patch - 1) == 0
    if not (central and powers and nchan == 4 and slab % 16 == 0 and positions.shape[0] % 8 == 0 and positions.shape[0] <= LANES):
        return on_any_device(residual, psf, positions)
    positions = positions.T
    start, couple = make_tables(positions, residual, psf)
    win, amps = gather_patch(nchan, nrows, psf, start, couple)
    image = apply_peaks(positions, amps, residual, win)
    return (image, sum_channels(nchan, nrows, image))


def on_any_device(residual, psf, positions):
    chan_id = lax.axis_index("chan")
    nchan = lax.axis_size("chan")
    row_id = lax.axis_index("rows")
    nrows = lax.axis_size("rows")
    slab = residual.shape[1]
    ncols = residual.shape[2]
    own_psf = psf[0]
    shard_rows = own_psf.shape[0]
    patch = own_psf.shape[1]
    half = patch // 2
    first = row_id * slab
    chan_hot = (jnp.arange(nchan) == chan_id).astype(jnp.float32)
    full_psf = lax.all_gather(own_psf, "rows", axis=0, tiled=True)
    padded_psf = jnp.pad(full_psf, ((slab, slab), (0, 0)))
    zero = jnp.int32(0)

    def subtract(image, row, col, amount):
        offset = first - row + half
        touches = jnp.logical_and(offset > -slab, offset < patch)
        start = jnp.clip(offset + slab, 0, patch + slab)
        psf_rows = lax.dynamic_slice(padded_psf, (start, zero), (slab, patch))
        window = lax.dynamic_slice(image, (zero, col - half), (slab, patch))
        scale = jnp.where(touches, amount, 0.0)
        return lax.dynamic_update_slice(image, window - scale * psf_rows, (zero, col - half))

    image = residual[0]
    peak_rows = positions[:, 0]
    peak_cols = positions[:, 1]
    inside = jnp.logical_and(peak_rows >= first, peak_rows < first + slab)
    local_rows = jnp.clip(peak_rows - first, 0, slab - 1)
    start_values = jnp.where(inside, image[local_rows, peak_cols], 0.0)
    row_offset = peak_rows[:, None] - peak_rows[None, :] + half - row_id * shard_rows
    col_offset = peak_cols[:, None] - peak_cols[None, :] + half
    owned = (row_offset >= 0) & (row_offset < shard_rows) & (col_offset >= 0) & (col_offset < patch)
    couple = own_psf[jnp.clip(row_offset, 0, shard_rows - 1), jnp.clip(col_offset, 0, patch - 1)]
    couple = jnp.where(owned, couple, 0.0)
    start_table, couple_table = lax.psum(
        (chan_hot[:, None] * start_values[None, :], chan_hot[:, None, None] * couple[None, :, :]),
        ("chan", "rows"),
    )

    def solve(k, amps):
        taken = jnp.sum(amps * lax.dynamic_index_in_dim(couple_table, k, 1, False), axis=1)
        value = lax.dynamic_index_in_dim(start_table, k, 1, False) - taken
        amp = 0.25 * (value + jnp.sum(value) / nchan)
        return lax.dynamic_update_index_in_dim(amps, amp, k, 1)

    amps = lax.fori_loop(0, STEPS, solve, jnp.zeros((nchan, STEPS), jnp.float32))
    own_amps = jnp.sum(chan_hot[:, None] * amps, axis=0)

    def apply(k, image):
        return subtract(image, positions[k, 0], positions[k, 1], own_amps[k])

    image = lax.fori_loop(0, STEPS, apply, image)
    count = slab * nrows * ncols
    parts = lax.psum_scatter(image, "chan", scatter_dimension=1, tiled=True)
    total = lax.psum(jnp.sum(parts * parts), ("chan", "rows"))
    normalized = parts * lax.rsqrt(total / count + 1e-06)
    return (image[None], normalized)


def solution(mesh):
    return jax.shard_map(
        on_device,
        mesh=mesh,
        in_specs=(P("chan", "rows", None), P("chan", "rows", None), P()),
        out_specs=(P("chan", "rows", None), P("rows", "chan")),
        check_vma=False,
    )
```
